32 devices in a mesh: gx: 2 (over y), gy: 4 (over x, core), gz: 4 (over z).
Axes of the slice: x: 2, y: 2, z: 4, core: 2. Of those that a mesh axis runs over, the one named last changes fastest.
Arguments:
- offsets: float32 [4, 8, 32, 16, 3], P('gx', 'gy', 'gz'), may hold values from 0.2649 to 2.3351, as said below
- velocities: float32 [4, 8, 32, 16, 3], P('gx', 'gy', 'gz'), may hold values from -6 to 6
- occupied: int32 [4, 8, 32, 16], P('gx', 'gy', 'gz'), may hold values 0 or 1
Outputs:
- positions: float32 [4, 8, 32, 16, 3], P('gx', 'gy', 'gz')
- new_velocities: float32 [4, 8, 32, 16, 3], P('gx', 'gy', 'gz')
- forces: float32 [4, 8, 32, 16, 3], P('gx', 'gy', 'gz')
- capacity_history: float32 [4, 2], replicated
The draws below stay inside these ranges and needn't reach their ends.
Inputs may be any that keep to these rules, and one draw needn't show every extreme that they name: `offsets`: each offset lies within the cell, a jittered body-centred lattice of 16 sites with spacing 1.3 per cell, jitter at most 0.06 in each coordinate.
All inputs are finite; a program needn't handle non-finite values.
Results may differ from the reference program's by a relative error of at most 0.0003.
Values sent between devices are 32-bit elements.
A program may use at most 128 MiB of HBM per device.

```python
import jax
import jax.numpy as jnp
from jax import lax

SLOTS = 16
STEPS = 4
NX = 4
NY = 8
NZ = 32


LATTICE_STEP = 1.3


JITTER = 0.06


def draw_offsets(key, part):
    slot_ids = jnp.arange(SLOTS) % 16
    corner = slot_ids % 8
    corner_bits = jnp.stack([corner // 4, corner // 2 % 2, corner % 2], axis=-1).astype(jnp.float32)
    centred = (slot_ids // 8).astype(jnp.float32)[:, None]
    lattice = LATTICE_STEP * (corner_bits + 0.5 * centred) + 0.325
    shape_all = (NX, NY, NZ, SLOTS, 3)
    jitter = jax.random.uniform(key, shape_all, jnp.float32, -JITTER, JITTER)
    return (lattice + jitter).astype(jnp.float32)


def plant(result, key, smallest, largest):
    longest = result.shape.index(max(result.shape))
    spots = []
    for shift in (0, 1):
        where = [jax.random.randint(jax.random.fold_in(key, axis), (), 0, length) for axis, length in enumerate(result.shape)]
        where[longest] = (where[longest] + shift) % result.shape[longest]
        spots.append(tuple(where))
    return result.at[spots[0]].set(smallest).at[spots[1]].set(largest)


def block_levels(stream_key, dims, pieces, least, largest):
    def one(dim, shards_of):
        heights = jax.random.uniform(jax.random.fold_in(jax.random.fold_in(stream_key, 6), dim), (shards_of,), jnp.float32, least / len(pieces), largest / len(pieces))
        return jnp.repeat(jnp.exp(heights), dims[dim] // shards_of).reshape((-1,) + (1,) * (len(dims) - dim - 1))

    loudness = one(*pieces[0])
    for cut in pieces[1:]:
        loudness = loudness * one(*cut)
    return loudness


def bell_draw(own_key, shape, spread, bound, shards=(), kind=jnp.bfloat16):
    level = block_levels(own_key, shape, shards, -0.22, 0.18) if shards else 1.0
    entries = jax.random.normal(own_key, shape, jnp.float32) * spread * level
    return jnp.minimum(jnp.maximum(entries, -bound), bound).astype(kind)


def setup_inputs(seed: int = 0) -> dict:
    keys = jax.random.split(jax.random.key(seed), 4)
    offsets = draw_offsets(jax.random.fold_in(keys[3], 71), 0)
    velocities = bell_draw(keys[1], (NX, NY, NZ, SLOTS, 3), 1.0, 6.0, ((0, 2), (1, 4), (2, 4)), jnp.float32)
    occupied = plant((jax.random.randint(keys[2], (NX, NY, NZ, SLOTS), 0, 16) < 13).astype(jnp.int32), jax.random.fold_in(keys[2], 1), 0, 1)
    return dict(offsets=offsets, velocities=velocities, occupied=occupied)


CUTOFF = 2.5
CELL_SIDE = 2.6
TIME_STEP = 0.005
BATH_STRENGTH = 0.25
GOAL_WARMTH = 0.8
FORCE_EDGE = 24.0 * (2.0 * CUTOFF ** (-13) - CUTOFF ** (-7))
ENERGY_EDGE = 4.0 * (CUTOFF ** (-12) - CUTOFF ** (-6))
STENCILS = [(along_x, along_y, along_z) for along_x in (-1, 0, 1) for along_y in (-1, 0, 1) for along_z in (-1, 0, 1)]

def pair_terms(own_cells, neighbour, stencil):
    cell_shift = jnp.array(stencil, jnp.float32) * CELL_SIDE
    separation = neighbour[..., None, :, :3] + cell_shift - own_cells[..., :, None, :3]
    squared = lax.optimization_barrier(jnp.sum(separation * separation, axis=-1))
    occupied_pair = own_cells[..., :, None, 3] * neighbour[..., None, :, 3]
    inside = (occupied_pair > 0.5) & (squared < CUTOFF * CUTOFF)
    if stencil == (0, 0, 0):
        slots_count = own_cells.shape[-2]
        inside = inside & jnp.logical_not(jnp.eye(slots_count, dtype=bool))
    guarded = jnp.where(inside, squared, 1.0)
    inverse = 1.0 / guarded
    inverse_six = inverse * inverse * inverse
    radius = jnp.sqrt(guarded)
    strength = 24.0 * (2.0 * inverse_six * inverse_six - inverse_six) * inverse - FORCE_EDGE / radius
    strength = jnp.where(inside, strength, 0.0)
    energy = 4.0 * (inverse_six * inverse_six - inverse_six) - ENERGY_EDGE + (radius - CUTOFF) * FORCE_EDGE
    energy = jnp.where(inside, energy, 0.0)
    pushes = -strength[..., None] * separation
    return (pushes, energy)

def window(padded, stencil, extent):
    return padded[1 + stencil[0]:1 + stencil[0] + extent[0], 1 + stencil[1]:1 + stencil[1] + extent[1], 1 + stencil[2]:1 + stencil[2] + extent[2]]

def full_forces(padded):
    extent = (padded.shape[0] - 2, padded.shape[1] - 2, padded.shape[2] - 2)
    own_cells = window(padded, (0, 0, 0), extent)
    forces = jnp.zeros(own_cells.shape[:-1] + (3,), jnp.float32)
    energy = jnp.zeros((), jnp.float32)
    for stencil in STENCILS:
        pushes, pair_energy = pair_terms(own_cells, window(padded, stencil, extent), stencil)
        forces = forces + lax.optimization_barrier(jnp.sum(pushes, axis=-2))
        energy = energy + jnp.sum(pair_energy)
    return (forces, 0.5 * energy)

def evaluate(position, weight):
    packed = jnp.concatenate([position, weight[..., None]], axis=-1)
    padded = jnp.pad(packed, ((1, 1), (1, 1), (1, 1), (0, 0), (0, 0)), mode='wrap')

    def one_plane(plane_index):
        block = lax.dynamic_slice_in_dim(padded, plane_index, 3, 0)
        return full_forces(block)
    forces, capacity_history = lax.map(one_plane, jnp.arange(NX, dtype=jnp.int32))
    return (forces.reshape(position.shape), jnp.sum(capacity_history))

def reference(offsets, velocities, occupied):
    weight = occupied.astype(jnp.float32)
    velocity = velocities * weight[..., None]
    position = offsets
    slot_total = float(NX * NY * NZ * SLOTS)
    forces, initial_energy = evaluate(position, weight)
    body_tally = jnp.sum(weight)
    records = []
    for step_index in range(STEPS):
        velocity = velocity + 0.5 * TIME_STEP * forces
        position = position + TIME_STEP * velocity
        forces, potential = evaluate(position, weight)
        velocity = velocity + 0.5 * TIME_STEP * forces
        moving_vigor = 0.5 * jnp.sum(velocity * velocity)
        warmth_gauge = 2.0 * moving_vigor / (3.0 * body_tally)
        speed_stretch = jnp.sqrt(1.0 + BATH_STRENGTH * (GOAL_WARMTH / warmth_gauge - 1.0))
        velocity = speed_stretch * velocity
        records.append(jnp.stack([potential, speed_stretch * speed_stretch * moving_vigor]) / slot_total)
    return (position, velocity, forces, jnp.stack(records))
```

```python
import functools

import jax
import jax.numpy as jnp
from jax import lax
from jax.experimental import pallas as pl
from jax.experimental.pallas import tpu as pltpu
from jax.sharding import PartitionSpec as P

MESH = pl.DeviceIdType.MESH
STEPS = 4
CUTOFF = 2.5
CELL_SIDE = 2.6
TIME_STEP = 0.005
BATH_STRENGTH = 0.25
GOAL_WARMTH = 0.8
FORCE_EDGE = 24.0 * (2.0 * CUTOFF ** (-13) - CUTOFF ** (-7))
ENERGY_EDGE = 4.0 * (CUTOFF ** (-12) - CUTOFF ** (-6))
FAR = 1.0e15


def offsets_of(size):
    return [0] if size == 1 else [0, 1] if size == 2 else [0, 1, -1]


def kernel(
    axes, shape, o_in, v_in, occ_in, o_out, v_out, f_out, h_out,
    ostate, vstate, near, osend, orecv, fsend, frecv, kbuf, tally, stretch,
    o_send_sem, o_recv_sem, f_send_sem, f_recv_sem, k_send_sem, k_recv_sem,
):
    gx, gy, gz = axes
    nx, ny, nz, slots = shape
    lanes = nz * slots
    tile = fsend.shape[2]
    devices = gx * gy * gz
    slot_total = float(devices * nx * ny * lanes)
    me = [lax.axis_index(a) for a in ("gx", "gy", "gz")]
    my_id = (me[0] * gy + me[1]) * gz + me[2]

    def device(j):
        d = lax.rem(my_id + j, devices)
        return (d // (gy * gz), lax.rem(d // gz, gy), lax.rem(d, gz))

    def canonical(size, off):
        return 0 if size == 1 else off % 2 if size == 2 else off

    def padded(size, n):
        return (
            [(canonical(size, -1), n - 1)]
            + [(0, i) for i in range(n)]
            + [(canonical(size, 1), 0)]
        )

    px_of, py_of = padded(gx, nx), padded(gy, ny)
    xs = offsets_of(gx)
    partners = [
        (a, b, c) for a in xs for b in offsets_of(gy) for c in offsets_of(gz) if (a, b, c) != (0, 0, 0)
    ]
    slot_of = {d: i for i, d in enumerate(partners)}

    def layers_of(b):
        return sorted({yl for off, yl in py_of if off == b})

    def halo_copies(src, dst, send_sem, recv_sem):
        copies = []
        for i, (a, b, c) in enumerate(partners):
            to = (
                lax.rem(me[0] - a + gx, gx), lax.rem(me[1] - b + gy, gy), lax.rem(me[2] - c + gz, gz),
            )
            need = layers_of(b)
            where = pl.ds(need[0], need[-1] - need[0] + 1)
            copies.append(
                pltpu.make_async_remote_copy(
                    src_ref=src.at[where], dst_ref=dst.at[i, where],
                    send_sem=send_sem.at[i], recv_sem=recv_sem.at[i],
                    device_id=to, device_id_type=MESH,
                )
            )
        return copies

    barrier = pltpu.get_barrier_semaphore()

    def greet(j, _):
        pl.semaphore_signal(barrier, inc=1, device_id=device(j), device_id_type=MESH)
        return 0

    lax.fori_loop(1, devices, greet, 0)

    lane = lax.broadcasted_iota(jnp.int32, (nz, lanes), 1)
    level = lax.broadcasted_iota(jnp.int32, (nz, lanes), 0)
    spread = (
        lax.rem(lax.broadcasted_iota(jnp.int32, (slots, lanes), 1), slots)
        == lax.broadcasted_iota(jnp.int32, (slots, lanes), 0)
    ).astype(jnp.float32)

    def rows_of(planes):
        flat = planes.reshape(-1, slots)
        wide = jnp.dot(flat, spread, precision=lax.Precision.HIGHEST, preferred_element_type=jnp.float32)
        wide = wide.reshape(-1, nz, lanes)
        return jnp.sum(jnp.where((lane // slots == level)[None], wide, 0.0), axis=1)

    o_rows = rows_of(o_in[...])
    v_rows = rows_of(v_in[...])
    w_rows = rows_of(occ_in[...].astype(jnp.float32))
    osend[...] = jnp.zeros_like(osend)
    fsend[...] = jnp.zeros_like(fsend)
    for x in range(nx):
        for y in range(ny):
            w = w_rows[x * ny + y : x * ny + y + 1]
            for c in range(3):
                i = (x * ny + y) * 3 + c
                r = c * nx + x
                osend[y, 0, r : r + 1] = jnp.where(w > 0.5, o_rows[i : i + 1], FAR)
                osend[y, 1, r : r + 1] = v_rows[i : i + 1] * w
    tally[...] = jnp.sum(w_rows, axis=0, keepdims=True)

    pl.semaphore_wait(barrier, devices - 1)
    first = halo_copies(osend, orecv, o_send_sem, o_recv_sem)
    for copy in first:
        copy.start()
    for copy in first:
        copy.wait()

    edge_lane = lax.broadcasted_iota(jnp.int32, (tile, lanes), 1)

    def columns(own, received):
        found = {}
        for xi, a in enumerate(xs):
            for py, (b, yl) in enumerate(py_of):
                def block(c):
                    d = (a, b, canonical(gz, c))
                    return own(yl) if d == (0, 0, 0) else received(slot_of[d], yl)

                mid = block(0)
                found[xi, py, 1] = mid
                low = jnp.where(edge_lane >= lanes - slots, block(-1), mid)
                found[xi, py, 0] = pltpu.roll(low, slots, 1)
                high = jnp.where(edge_lane < slots, block(1), mid)
                found[xi, py, 2] = pltpu.roll(high, lanes - slots, 1)
        return found

    for q, state in enumerate((ostate, vstate)):
        found = columns(lambda yl: osend[yl, q], lambda s, yl: orecv[s, yl, q])
        for (xi, py, dz), value in found.items():
            state[xi, py, dz] = value

    row_id = lax.broadcasted_iota(jnp.int32, (2 * 8, lanes), 0)
    lane_id = lax.broadcasted_iota(jnp.int32, (slots, lanes), 1)
    slot_id = lax.broadcasted_iota(jnp.int32, (slots, lanes), 0)
    pick = (lane_id // slots) * slots + slot_id
    itself = lax.rem(lane_id, slots) == slot_id

    def nearby(py, _):
        for px, (a, xl) in enumerate(px_of):
            for dz in range(3):
                block = ostate[xs.index(a), py, dz]
                for c in range(3):
                    r = c * nx + xl
                    row = jnp.broadcast_to(block[r : r + 1], (slots, lanes))
                    near[px, py, dz, c] = jnp.take_along_axis(row, pick, axis=1, mode="promise_in_bounds")
        return 0

    def out_planes(block, ref, y, mask):
        at = lax.broadcasted_iota(jnp.int32, (nz, lanes), 0) * slots + lax.rem(lane, slots)
        for x in range(nx):
            for c in range(3):
                r = c * nx + x
                row = jnp.broadcast_to(block[r : r + 1], (nz, lanes))
                plane = jnp.take_along_axis(row, at, axis=1, mode="promise_in_bounds")[:, :slots]
                if mask:
                    plane = jnp.where(occ_in[x, y] > 0, plane, o_in[x, y, c])
                ref[x, y, c] = plane

    half = 0.5 * TIME_STEP

    def step(k, _):
        p = lax.rem(k, 2)
        lax.fori_loop(0, ny + 2, nearby, 0)

        energy_rows = jnp.zeros((1, lanes), jnp.float32)
        for x in range(nx):
            def one_row(y, carried):
                block = ostate[0, y + 1, 1]
                mine = [block[c * nx + x : c * nx + x + 1] for c in range(3)]
                occupied = mine[0] < 0.5 * FAR
                force = [jnp.zeros((slots, lanes), jnp.float32) for _ in range(3)]
                energy = jnp.zeros((slots, lanes), jnp.float32)
                for dx in (-1, 0, 1):
                    for dy in (-1, 0, 1):
                        for dz in (-1, 0, 1):
                            shift = (dx, dy, dz)
                            apart = [
                                near[x + 1 + dx, y + 1 + dy, dz + 1, c] - (mine[c] - shift[c] * CELL_SIDE)
                                for c in range(3)
                            ]
                            squared = apart[0] * apart[0] + apart[1] * apart[1] + apart[2] * apart[2]
                            if shift == (0, 0, 0):
                                squared = jnp.where(itself, FAR, squared)
                            inside = squared < CUTOFF * CUTOFF
                            inv = lax.rsqrt(squared)
                            inv2 = inv * inv
                            inv6 = inv2 * inv2 * inv2
                            pull = inv * (FORCE_EDGE - inv * inv6 * (48.0 * inv6 - 24.0))
                            pull = jnp.where(inside, pull, 0.0)
                            for c in range(3):
                                force[c] = force[c] + pull * apart[c]
                            bond = inv6 * (4.0 * inv6 - 4.0) + (
                                squared * inv * FORCE_EDGE - (ENERGY_EDGE + CUTOFF * FORCE_EDGE)
                            )
                            energy = energy + jnp.where(inside, bond, 0.0)
                for c in range(3):
                    total = jnp.sum(force[c], axis=0, keepdims=True)
                    fsend[p, y, c * nx + x : c * nx + x + 1] = jnp.where(occupied, total, 0.0)
                total = jnp.sum(energy, axis=0, keepdims=True)
                return carried + jnp.where(occupied, total, 0.0)

            energy_rows = lax.fori_loop(0, ny, one_row, energy_rows)

        kinetic = jnp.zeros((tile, lanes), jnp.float32)
        for y in range(ny):
            v = vstate[0, y + 1, 1] + half * fsend[p, y]
            kinetic = kinetic + v * v
        kinetic = 0.5 * jnp.sum(kinetic, axis=0, keepdims=True)
        kbuf[p, my_id, 0:1] = jnp.where(k == 0, tally[...], kinetic)
        kbuf[p, my_id, 1:2] = 0.5 * energy_rows

        def k_copy(j):
            return pltpu.make_async_remote_copy(
                src_ref=kbuf.at[p, my_id], dst_ref=kbuf.at[p, my_id],
                send_sem=k_send_sem.at[j - 1], recv_sem=k_recv_sem.at[p, j - 1],
                device_id=device(j), device_id_type=MESH,
            )

        def start(j, _):
            k_copy(j).start()
            return 0

        def finish(j, _):
            k_copy(j).wait()
            return 0

        halo = halo_copies(fsend.at[p], frecv.at[p], f_send_sem, f_recv_sem.at[p])

        @pl.when(k < STEPS)
        def _():
            for copy in halo:
                copy.start()

        lax.fori_loop(1, devices, start, 0)

        @pl.when(k == STEPS)
        def _():
            for y in range(ny):
                out_planes(ostate[0, y + 1, 1], o_out, y, True)
                out_planes(fsend[p, y], f_out, y, False)

        lax.fori_loop(1, devices, finish, 0)

        @pl.when(k < STEPS)
        def _():
            for copy in halo:
                copy.wait()

        everyone = jnp.sum(kbuf[p], axis=0)
        totals = jnp.sum(everyone, axis=1, keepdims=True)
        vigor, potential = totals[0:1], totals[1:2]

        @pl.when(k == 0)
        def _():
            tally[...] = jnp.broadcast_to(vigor, (1, lanes))
            stretch[...] = jnp.ones_like(stretch)

        @pl.when(k > 0)
        def _():
            warmth = 2.0 * jnp.broadcast_to(vigor, (1, lanes)) / (3.0 * tally[...])
            lam = jnp.sqrt(1.0 + BATH_STRENGTH * (GOAL_WARMTH / warmth - 1.0))
            stretch[...] = lam
            which = lax.broadcasted_iota(jnp.int32, (1, lanes), 1)
            record = jnp.where(which == 0, potential, lam * lam * vigor) / slot_total
            h_out[pl.ds(k - 1, 1), :] = record[:, :2]

        lam = stretch[...]
        before = jnp.where(k > 0, half, 0.0)

        @pl.when(k < STEPS)
        def _():
            found = columns(lambda yl: fsend[p, yl], lambda s, yl: frecv[p, s, yl])
            for (xi, py, dz), f in found.items():
                v = (vstate[xi, py, dz] + before * f) * lam
                v = v + half * f
                vstate[xi, py, dz] = v
                ostate[xi, py, dz] = ostate[xi, py, dz] + TIME_STEP * v

        @pl.when(k == STEPS)
        def _():
            for y in range(ny):
                v = (vstate[0, y + 1, 1] + half * fsend[p, y]) * lam
                out_planes(v, v_out, y, False)

        return 0

    lax.fori_loop(0, STEPS + 1, step, 0)


def shards(axes, offsets, velocities, occupied):
    gx, gy, gz = axes
    nx, ny, nz, slots = occupied.shape
    lanes = nz * slots
    tile = -(-3 * nx // 8) * 8
    nxo, nyo, nzo = (len(offsets_of(s)) for s in axes)
    halo = nxo * nyo * nzo - 1
    devices = gx * gy * gz
    f32 = jnp.float32
    plane = jax.ShapeDtypeStruct((nx, ny, 3, nz, slots), f32)
    vmem = pl.BlockSpec(memory_space=pltpu.VMEM)
    dma = pltpu.SemaphoreType.DMA
    o, v, f, h = pl.pallas_call(
        functools.partial(kernel, axes, (nx, ny, nz, slots)),
        name="verlet",
        out_shape=[plane, plane, plane, jax.ShapeDtypeStruct((STEPS, 2), f32)],
        in_specs=[vmem] * 3,
        out_specs=[vmem] * 4,
        scratch_shapes=[
            pltpu.VMEM((nxo, ny + 2, 3, tile, lanes), f32),
            pltpu.VMEM((nxo, ny + 2, 3, tile, lanes), f32),
            pltpu.VMEM((nx + 2, ny + 2, 3, 3, slots, lanes), f32),
            pltpu.VMEM((ny, 2, tile, lanes), f32),
            pltpu.VMEM((halo, ny, 2, tile, lanes), f32),
            pltpu.VMEM((2, ny, tile, lanes), f32),
            pltpu.VMEM((2, halo, ny, tile, lanes), f32),
            pltpu.VMEM((2, devices, 2, lanes), f32),
            pltpu.VMEM((1, lanes), f32),
            pltpu.VMEM((1, lanes), f32),
            dma((halo,)),
            dma((halo,)),
            dma((halo,)),
            dma((2, halo)),
            dma((devices - 1,)),
            dma((2, devices - 1)),
        ],
        compiler_params=pltpu.CompilerParams(collective_id=0, has_side_effects=True),
    )(
        jnp.transpose(offsets, (0, 1, 4, 2, 3)),
        jnp.transpose(velocities, (0, 1, 4, 2, 3)),
        occupied,
    )
    back = (0, 1, 3, 4, 2)
    return (jnp.transpose(o, back), jnp.transpose(v, back), jnp.transpose(f, back), h)


def solution(mesh):
    axes = tuple(mesh.shape[a] for a in ("gx", "gy", "gz"))
    in_specs = (
        P("gx", "gy", "gz", None, None),
        P("gx", "gy", "gz", None, None),
        P("gx", "gy", "gz", None),
    )
    out_specs = (
        P("gx", "gy", "gz", None, None),
        P("gx", "gy", "gz", None, None),
        P("gx", "gy", "gz", None, None),
        P(),
    )
    return jax.shard_map(
        functools.partial(shards, axes), mesh=mesh, in_specs=in_specs, out_specs=out_specs, check_vma=False
    )
```

```python
import functools

import jax
import jax.numpy as jnp
from jax import lax
from jax.experimental import pallas as pl
from jax.experimental.pallas import tpu as pltpu
from jax.sharding import PartitionSpec as P

MESH = pl.DeviceIdType.MESH
STEPS = 4
CUTOFF = 2.5
CELL_SIDE = 2.6
TIME_STEP = 0.005
BATH_STRENGTH = 0.25
GOAL_WARMTH = 0.8
FORCE_EDGE = 24.0 * (2.0 * CUTOFF ** (-13) - CUTOFF ** (-7))
ENERGY_EDGE = 4.0 * (CUTOFF ** (-12) - CUTOFF ** (-6))
FAR = 1.0e15


def offsets_of(size):
    return [0] if size == 1 else [0, 1] if size == 2 else [0, 1, -1]


def kernel(
    axes, shape, o_in, v_in, occ_in, o_out, v_out, f_out, h_out,
    ostate, vstate, near, osend, orecv, oedge, oedges, fsend, frecv, fedge, fedges, tally, history,
    o_send_sem, o_recv_sem, f_send_sem, f_recv_sem,
):
    gx, gy, gz = axes
    nx, ny, nz, slots = shape
    lanes = nz * slots
    tile = fsend.shape[2]
    devices = gx * gy * gz
    slot_total = float(devices * nx * ny * lanes)
    me = [lax.axis_index(a) for a in ("gx", "gy", "gz")]
    my_id = (me[0] * gy + me[1]) * gz + me[2]

    turned = [[lax.rem(me[i] + j, n) for j in range(n)] for i, n in enumerate(axes)]

    def device(d):
        return tuple(turned[i][d[i] % axes[i]] for i in range(3))

    def id_of(d):
        at = device(d)
        return (at[0] * gy + at[1]) * gz + at[2]

    def canonical(size, off):
        return 0 if size == 1 else off % 2 if size == 2 else off

    def padded(size, n):
        return (
            [(canonical(size, -1), n - 1)]
            + [(0, i) for i in range(n)]
            + [(canonical(size, 1), 0)]
        )

    px_of, py_of = padded(gx, nx), padded(gy, ny)
    xs = offsets_of(gx)
    partners = [
        (a, b, c) for a in xs for b in offsets_of(gy) for c in offsets_of(gz) if (a, b, c) != (0, 0, 0)
    ]
    slot_of = {d: i for i, d in enumerate(partners)}
    met = {tuple(o % n for o, n in zip(d, axes)) for d in partners}
    far = [
        (a, b, c) for a in range(gx) for b in range(gy) for c in range(gz)
        if (a, b, c) not in met and (a, b, c) != (0, 0, 0)
    ]
    level_of = [i for i, d in enumerate(partners) if d[2] == 0]
    level_slot = {partners[i]: j for j, i in enumerate(level_of)}

    def layers_of(b):
        return sorted({yl for off, yl in py_of if off == b})

    def copies_of(send, recv, edge, edge_at, send_sem, recv_sem, with_far):
        copies = []
        for i, d in enumerate(far if with_far else []):
            copies.append((edge.at[0, pl.ds(0, 1)], edge_at(d, 1), len(partners) + i, d))
        for i, d in reversed([*enumerate(partners)]):
            need = layers_of(d[1])
            where = pl.ds(need[0], len(need))
            if d[2] == 0:
                copies.append((send.at[where], recv.at[level_slot[d], where], i, d))
            else:
                copies.append((edge.at[0 if d[2] == 1 else 1, where], edge_at(d, len(need)), i, d))
        return [
            pltpu.make_async_remote_copy(
                src_ref=src, dst_ref=dst, send_sem=send_sem.at[i], recv_sem=recv_sem.at[i],
                device_id=device(tuple(-x for x in d)), device_id_type=MESH,
            )
            for src, dst, i, d in copies
        ]

    barrier = pltpu.get_barrier_semaphore()

    for d in far + partners:
        pl.semaphore_signal(barrier, inc=1, device_id=device(d), device_id_type=MESH)

    lane = lax.broadcasted_iota(jnp.int32, (nz, lanes), 1)
    level = lax.broadcasted_iota(jnp.int32, (nz, lanes), 0)
    spread = (
        lax.rem(lax.broadcasted_iota(jnp.int32, (slots, lanes), 1), slots)
        == lax.broadcasted_iota(jnp.int32, (slots, lanes), 0)
    ).astype(jnp.float32)

    def rows_of(planes):
        flat = planes.reshape(-1, slots)
        wide = jnp.dot(flat, spread, precision=lax.Precision.HIGHEST, preferred_element_type=jnp.float32)
        wide = wide.reshape(-1, nz, lanes)
        return jnp.sum(jnp.where((lane // slots == level)[None], wide, 0.0), axis=1)

    o_rows = rows_of(o_in[...])
    v_rows = rows_of(v_in[...])
    w_rows = rows_of(occ_in[...].astype(jnp.float32))
    osend[...] = jnp.zeros_like(osend)
    fsend[...] = jnp.zeros_like(fsend)
    for x in range(nx):
        for y in range(ny):
            w = w_rows[x * ny + y : x * ny + y + 1]
            for c in range(3):
                i = (x * ny + y) * 3 + c
                r = c * nx + x
                osend[y, 0, r : r + 1] = jnp.where(w > 0.5, o_rows[i : i + 1], FAR)
                osend[y, 1, r : r + 1] = v_rows[i : i + 1] * w
    tally[...] = jnp.broadcast_to(jnp.sum(w_rows, keepdims=True), (1, lanes))

    tile_lane = lax.broadcasted_iota(jnp.int32, (tile, lanes), 1)
    tile_row = lax.broadcasted_iota(jnp.int32, (tile, lanes), 0)
    ends = [lax.rem(tile_lane, slots), lax.rem(tile_lane, slots) + (lanes - slots)]
    back = tile_row * slots + lax.rem(tile_lane, slots)

    def packed(block, side):
        taken = jnp.take_along_axis(block, ends[side], axis=1, mode="promise_in_bounds")
        return jnp.sum(jnp.where(tile_lane // slots == tile_row, taken, 0.0), axis=0, keepdims=True)

    def unpacked(row):
        wide = jnp.broadcast_to(row, (tile, lanes))
        return jnp.take_along_axis(wide, back, axis=1, mode="promise_in_bounds")

    for side in range(2):
        for y in range(ny):
            for q in range(2):
                oedge[side, y, q] = packed(osend[y, q], side)

    pl.semaphore_wait(barrier, devices - 1)
    first = copies_of(
        osend, orecv, oedge, lambda d, n: oedges.at[slot_of[d], pl.ds(0, n)], o_send_sem, o_recv_sem, False
    )
    for copy in first:
        copy.start()
    for copy in first:
        copy.wait()

    edge_lane = tile_lane

    def columns(own, level_block, edge_row):
        found = {}
        for xi, a in enumerate(xs):
            for py, (b, yl) in enumerate(py_of):
                mid = own(yl) if (a, b) == (0, 0) else level_block(level_slot[a, b, 0], yl)
                found[xi, py, 1] = mid
                at = layers_of(b).index(yl)
                below, above = (unpacked(edge_row((a, b, c), at)) for c in (-1, 1))
                low = jnp.where(edge_lane >= lanes - slots, below, mid)
                found[xi, py, 0] = pltpu.roll(low, slots, 1)
                high = jnp.where(edge_lane < slots, above, mid)
                found[xi, py, 2] = pltpu.roll(high, lanes - slots, 1)
        return found

    for q, state in enumerate((ostate, vstate)):
        found = columns(
            lambda yl: osend[yl, q], lambda s, yl: orecv[s, yl, q], lambda d, at: oedges[slot_of[d], at, q]
        )
        for (xi, py, dz), value in found.items():
            state[xi, py, dz] = value

    lane_id = lax.broadcasted_iota(jnp.int32, (slots, lanes), 1)
    slot_id = lax.broadcasted_iota(jnp.int32, (slots, lanes), 0)
    pick = (lane_id // slots) * slots + slot_id
    itself = lax.rem(lane_id, slots) == slot_id

    def nearby(py, _):
        for px, (a, xl) in enumerate(px_of):
            for dz in range(3):
                block = ostate[xs.index(a), py, dz]
                for c in range(3):
                    r = c * nx + xl
                    row = jnp.broadcast_to(block[r : r + 1], (slots, lanes))
                    near[px, py, dz, c] = jnp.take_along_axis(row, pick, axis=1, mode="promise_in_bounds")
        return 0

    def out_planes(block, ref, y, mask):
        at = lax.broadcasted_iota(jnp.int32, (nz, lanes), 0) * slots + lax.rem(lane, slots)
        for x in range(nx):
            for c in range(3):
                r = c * nx + x
                row = jnp.broadcast_to(block[r : r + 1], (nz, lanes))
                plane = jnp.take_along_axis(row, at, axis=1, mode="promise_in_bounds")[:, :slots]
                if mask:
                    plane = jnp.where(occ_in[x, y] > 0, plane, o_in[x, y, c])
                ref[x, y, c] = plane

    half = 0.5 * TIME_STEP

    def step(k, _):
        p = lax.rem(k, 2)
        for py in range(ny + 2):
            nearby(py, 0)

        energy_rows = jnp.zeros((1, lanes), jnp.float32)
        for x in range(nx):
            def one_row(y, carried):
                block = ostate[0, y + 1, 1]
                mine = [block[c * nx + x : c * nx + x + 1] for c in range(3)]
                occupied = mine[0] < 0.5 * FAR
                force = [jnp.zeros((slots, lanes), jnp.float32) for _ in range(3)]
                energy = jnp.zeros((slots, lanes), jnp.float32)
                for dx in (-1, 0, 1):
                    for dy in (-1, 0, 1):
                        for dz in (-1, 0, 1):
                            shift = (dx, dy, dz)
                            apart = [
                                near[x + 1 + dx, y + 1 + dy, dz + 1, c] - (mine[c] - shift[c] * CELL_SIDE)
                                for c in range(3)
                            ]
                            squared = apart[0] * apart[0] + apart[1] * apart[1] + apart[2] * apart[2]
                            if shift == (0, 0, 0):
                                squared = jnp.where(itself, FAR, squared)
                            inside = squared < CUTOFF * CUTOFF
                            inv = lax.rsqrt(squared)
                            inv2 = inv * inv
                            inv6 = inv2 * inv2 * inv2
                            pull = inv * (FORCE_EDGE - inv * inv6 * (48.0 * inv6 - 24.0))
                            pull = jnp.where(inside, pull, 0.0)
                            for c in range(3):
                                force[c] = force[c] + pull * apart[c]
                            bond = inv6 * (4.0 * inv6 - 4.0) + (
                                squared * inv * FORCE_EDGE - (ENERGY_EDGE + CUTOFF * FORCE_EDGE)
                            )
                            energy = energy + jnp.where(inside, bond, 0.0)
                for c in range(3):
                    total = jnp.sum(force[c], axis=0, keepdims=True)
                    fsend[p, y, c * nx + x : c * nx + x + 1] = jnp.where(occupied, total, 0.0)
                total = jnp.sum(energy, axis=0, keepdims=True)
                return carried + jnp.where(occupied, total, 0.0)

            energy_rows = lax.fori_loop(0, ny, one_row, energy_rows)

        kinetic = jnp.zeros((tile, lanes), jnp.float32)
        for y in range(ny):
            v = vstate[0, y + 1, 1] + half * jnp.where(tile_row < 3 * nx, fsend[p, y], 0.0)
            kinetic = kinetic + v * v
        kinetic = 0.5 * jnp.sum(kinetic, keepdims=True)
        kinetic = jnp.where(k == 0, tally[...], jnp.broadcast_to(kinetic, (1, lanes)))
        potential = jnp.broadcast_to(0.5 * jnp.sum(energy_rows, keepdims=True), (1, lanes))
        numbers = jnp.where(lane[:1] < (tile - 1) * slots, kinetic, potential)
        fedges[p, my_id, 0] = numbers
        for y in range(ny):
            fsend[p, y, tile - 2 : tile - 1] = kinetic
            fsend[p, y, tile - 1 : tile] = potential
        for side in range(2):
            for y in range(ny):
                fedge[p, side, y] = packed(fsend[p, y], side)

        halo = copies_of(
            fsend.at[p], frecv.at[p], fedge.at[p], lambda d, n: fedges.at[p, my_id, pl.ds(0, n)],
            f_send_sem, f_recv_sem.at[p], True,
        )
        for copy in halo:
            copy.start()

        @pl.when(k == STEPS)
        def _():
            for y in range(ny):
                out_planes(ostate[0, y + 1, 1], o_out, y, True)
                out_planes(fsend[p, y], f_out, y, False)

        for copy in halo:
            copy.wait()

        for d in partners:
            if d[2] == 0:
                block = frecv[p, level_slot[d], layers_of(d[1])[0]]
                fedges[p, id_of(d), 0] = jnp.where(
                    lane[:1] < (tile - 1) * slots, block[tile - 2 : tile - 1], block[tile - 1 : tile]
                )
        parts = [fedges[p, d, 0] for d in range(devices)]
        while len(parts) > 1:
            parts = [sum(parts[i + 1 : i + 2], parts[i]) for i in range(0, len(parts), 2)]
        at = (tile - 2) * slots
        vigor = jnp.broadcast_to(parts[0][:, at : at + 1], (1, lanes))
        potential = jnp.broadcast_to(parts[0][:, lanes - 1 :], (1, lanes))
        count = jnp.where(k == 0, vigor, tally[...])
        tally[...] = count
        warmth = 2.0 * vigor / (3.0 * count)
        lam = jnp.where(k == 0, 1.0, jnp.sqrt(1.0 + BATH_STRENGTH * (GOAL_WARMTH / warmth - 1.0)))
        which = lax.broadcasted_iota(jnp.int32, (2, lanes), 1)
        record = jnp.concatenate([potential, lam * lam * vigor], axis=0) / slot_total
        history[...] = jnp.where(which == k - 1, record, history[...])
        before = jnp.where(k > 0, half, 0.0)

        @pl.when(k < STEPS)
        def _():
            found = columns(
                lambda yl: fsend[p, yl], lambda s, yl: frecv[p, s, yl],
                lambda d, at: fedges[p, id_of(d), at],
            )
            for (xi, py, dz), f in found.items():
                f = jnp.where(tile_row < 3 * nx, f, 0.0)
                v = (vstate[xi, py, dz] + before * f) * lam
                v = v + half * f
                vstate[xi, py, dz] = v
                ostate[xi, py, dz] = ostate[xi, py, dz] + TIME_STEP * v

        @pl.when(k == STEPS)
        def _():
            for y in range(ny):
                v = (vstate[0, y + 1, 1] + half * fsend[p, y]) * lam
                out_planes(v, v_out, y, False)
            h_out[...] = history[:, :STEPS]

        return 0

    history[...] = jnp.zeros_like(history)
    lax.fori_loop(0, STEPS + 1, step, 0)


def shards(axes, offsets, velocities, occupied):
    gx, gy, gz = axes
    nx, ny, nz, slots = occupied.shape
    lanes = nz * slots
    tile = lanes // slots
    assert gz > 2 and tile >= 3 * nx + 2
    nxo, nyo, nzo = (len(offsets_of(s)) for s in axes)
    halo = nxo * nyo * nzo - 1
    level = nxo * nyo - 1
    devices = gx * gy * gz
    f32 = jnp.float32
    plane = jax.ShapeDtypeStruct((nx, ny, 3, nz, slots), f32)
    vmem = pl.BlockSpec(memory_space=pltpu.VMEM)
    dma = pltpu.SemaphoreType.DMA
    o, v, f, h = pl.pallas_call(
        functools.partial(kernel, axes, (nx, ny, nz, slots)),
        name="verlet",
        out_shape=[plane, plane, plane, jax.ShapeDtypeStruct((2, STEPS), f32)],
        in_specs=[vmem] * 3,
        out_specs=[vmem] * 4,
        scratch_shapes=[
            pltpu.VMEM((nxo, ny + 2, 3, tile, lanes), f32),
            pltpu.VMEM((nxo, ny + 2, 3, tile, lanes), f32),
            pltpu.VMEM((nx + 2, ny + 2, 3, 3, slots, lanes), f32),
            pltpu.VMEM((ny, 2, tile, lanes), f32),
            pltpu.VMEM((max(level, 1), ny, 2, tile, lanes), f32),
            pltpu.VMEM((2, ny, 2, 1, lanes), f32),
            pltpu.VMEM((halo, ny, 2, 1, lanes), f32),
            pltpu.VMEM((2, ny, tile, lanes), f32),
            pltpu.VMEM((2, max(level, 1), ny, tile, lanes), f32),
            pltpu.VMEM((2, 2, ny, 1, lanes), f32),
            pltpu.VMEM((2, devices, ny, 1, lanes), f32),
            pltpu.VMEM((1, lanes), f32),
            pltpu.VMEM((2, lanes), f32),
            dma((halo,)),
            dma((halo,)),
            dma((devices - 1,)),
            dma((2, devices - 1)),
        ],
        compiler_params=pltpu.CompilerParams(collective_id=0, has_side_effects=True),
    )(
        jnp.transpose(offsets, (0, 1, 4, 2, 3)),
        jnp.transpose(velocities, (0, 1, 4, 2, 3)),
        occupied,
    )
    back = (0, 1, 3, 4, 2)
    return (jnp.transpose(o, back), jnp.transpose(v, back), jnp.transpose(f, back), h.T)


def solution(mesh):
    axes = tuple(mesh.shape[a] for a in ("gx", "gy", "gz"))
    in_specs = (
        P("gx", "gy", "gz", None, None),
        P("gx", "gy", "gz", None, None),
        P("gx", "gy", "gz", None),
    )
    out_specs = (
        P("gx", "gy", "gz", None, None),
        P("gx", "gy", "gz", None, None),
        P("gx", "gy", "gz", None, None),
        P(),
    )
    return jax.shard_map(
        functools.partial(shards, axes), mesh=mesh, in_specs=in_specs, out_specs=out_specs, check_vma=False
    )
```

```python
import functools

import jax
import jax.numpy as jnp
from jax import lax
from jax.experimental import pallas as pl
from jax.experimental.pallas import tpu as pltpu
from jax.sharding import PartitionSpec as P

MESH = pl.DeviceIdType.MESH
STEPS = 4
CUTOFF = 2.5
CELL_SIDE = 2.6
TIME_STEP = 0.005
BATH_STRENGTH = 0.25
GOAL_WARMTH = 0.8
FORCE_EDGE = 24.0 * (2.0 * CUTOFF ** (-13) - CUTOFF ** (-7))
ENERGY_EDGE = 4.0 * (CUTOFF ** (-12) - CUTOFF ** (-6))
FAR = 1.0e15


def offsets_of(size):
    return [0] if size == 1 else [0, 1] if size == 2 else [0, 1, -1]


def kernel(
    axes, shape, o_in, v_in, occ_in, o_out, v_out, f_out, h_out,
    ostate, vstate, near, osend, orecv, oedge, oedges, fsend, frecv, fedge, fedges, tally, history,
    o_send_sem, o_recv_sem, f_send_sem, f_recv_sem,
):
    gx, gy, gz = axes
    nx, ny, nz, slots = shape
    lanes = nz * slots
    tile = fsend.shape[2]
    devices = gx * gy * gz
    slot_total = float(devices * nx * ny * lanes)
    me = [lax.axis_index(a) for a in ("gx", "gy", "gz")]
    my_id = (me[0] * gy + me[1]) * gz + me[2]

    turned = [[lax.rem(me[i] + j, n) for j in range(n)] for i, n in enumerate(axes)]

    def device(d):
        return tuple(turned[i][d[i] % axes[i]] for i in range(3))

    def id_of(d):
        at = device(d)
        return (at[0] * gy + at[1]) * gz + at[2]

    def canonical(size, off):
        return 0 if size == 1 else off % 2 if size == 2 else off

    def padded(size, n):
        return (
            [(canonical(size, -1), n - 1)]
            + [(0, i) for i in range(n)]
            + [(canonical(size, 1), 0)]
        )

    px_of, py_of = padded(gx, nx), padded(gy, ny)
    xs = offsets_of(gx)
    partners = [
        (a, b, c) for a in xs for b in offsets_of(gy) for c in offsets_of(gz) if (a, b, c) != (0, 0, 0)
    ]
    slot_of = {d: i for i, d in enumerate(partners)}
    met = {tuple(o % n for o, n in zip(d, axes)) for d in partners}
    far = [
        (a, b, c) for a in range(gx) for b in range(gy) for c in range(gz)
        if (a, b, c) not in met and (a, b, c) != (0, 0, 0)
    ]
    level_of = [i for i, d in enumerate(partners) if d[2] == 0]
    level_slot = {partners[i]: j for j, i in enumerate(level_of)}

    def layers_of(b):
        return sorted({yl for off, yl in py_of if off == b})

    def copies_of(send, recv, edge, edge_at, send_sem, recv_sem, with_far):
        copies, remote = [], []
        for i, d in enumerate(far if with_far else []):
            remote.append((edge.at[0, pl.ds(0, 1)], edge_at(d, 1), len(partners) + i, d))
        for i, d in reversed([*enumerate(partners)]):
            need = layers_of(d[1])
            where = pl.ds(need[0], len(need))
            if d[2] == 0:
                copies.append((send.at[where], recv.at[level_slot[d], where], i, d))
            else:
                copies.append((edge.at[0 if d[2] == 1 else 1, where], edge_at(d, len(need)), i, d))
        return [[
            pltpu.make_async_remote_copy(
                src_ref=src, dst_ref=dst, send_sem=send_sem.at[i], recv_sem=recv_sem.at[i],
                device_id=device(tuple(-x for x in d)), device_id_type=MESH,
            )
            for src, dst, i, d in chosen
        ] for chosen in ((copies, remote) if with_far else (copies,))]

    barrier = pltpu.get_barrier_semaphore()

    greeted = partners if max(n // 2 for n in axes) <= 3 else far + partners
    for d in greeted:
        pl.semaphore_signal(barrier, inc=1, device_id=device(d), device_id_type=MESH)

    lane = lax.broadcasted_iota(jnp.int32, (nz, lanes), 1)
    level = lax.broadcasted_iota(jnp.int32, (nz, lanes), 0)
    spread = (
        lax.rem(lax.broadcasted_iota(jnp.int32, (slots, lanes), 1), slots)
        == lax.broadcasted_iota(jnp.int32, (slots, lanes), 0)
    ).astype(jnp.float32)

    def rows_of(planes):
        flat = planes.reshape(-1, slots)
        wide = jnp.dot(flat, spread, precision=lax.Precision.HIGHEST, preferred_element_type=jnp.float32)
        wide = wide.reshape(-1, nz, lanes)
        return jnp.sum(jnp.where((lane // slots == level)[None], wide, 0.0), axis=1)

    o_rows = rows_of(o_in[...])
    v_rows = rows_of(v_in[...])
    w_rows = rows_of(occ_in[...].astype(jnp.float32))
    osend[...] = jnp.zeros_like(osend)
    fsend[...] = jnp.zeros_like(fsend)
    for x in range(nx):
        for y in range(ny):
            w = w_rows[x * ny + y : x * ny + y + 1]
            for c in range(3):
                i = (x * ny + y) * 3 + c
                r = c * nx + x
                osend[y, 0, r : r + 1] = jnp.where(w > 0.5, o_rows[i : i + 1], FAR)
                osend[y, 1, r : r + 1] = v_rows[i : i + 1] * w
    tally[...] = jnp.broadcast_to(jnp.sum(w_rows, keepdims=True), (1, lanes))

    tile_lane = lax.broadcasted_iota(jnp.int32, (tile, lanes), 1)
    tile_row = lax.broadcasted_iota(jnp.int32, (tile, lanes), 0)
    ends = [lax.rem(tile_lane, slots), lax.rem(tile_lane, slots) + (lanes - slots)]
    back = tile_row * slots + lax.rem(tile_lane, slots)

    def packed(block, side):
        taken = jnp.take_along_axis(block, ends[side], axis=1, mode="promise_in_bounds")
        return jnp.sum(jnp.where(tile_lane // slots == tile_row, taken, 0.0), axis=0, keepdims=True)

    def unpacked(row):
        wide = jnp.broadcast_to(row, (tile, lanes))
        return jnp.take_along_axis(wide, back, axis=1, mode="promise_in_bounds")

    for side in range(2):
        for y in range(ny):
            for q in range(2):
                oedge[side, y, q] = packed(osend[y, q], side)

    pl.semaphore_wait(barrier, len(greeted))
    (first,) = copies_of(
        osend, orecv, oedge, lambda d, n: oedges.at[slot_of[d], pl.ds(0, n)], o_send_sem, o_recv_sem, False
    )
    for copy in first:
        copy.start()
    for copy in first:
        copy.wait()

    edge_lane = tile_lane

    def columns(own, level_block, edge_row):
        found = {}
        for xi, a in enumerate(xs):
            for py, (b, yl) in enumerate(py_of):
                mid = own(yl) if (a, b) == (0, 0) else level_block(level_slot[a, b, 0], yl)
                found[xi, py, 1] = mid
                at = layers_of(b).index(yl)
                below, above = (unpacked(edge_row((a, b, c), at)) for c in (-1, 1))
                low = jnp.where(edge_lane >= lanes - slots, below, mid)
                found[xi, py, 0] = pltpu.roll(low, slots, 1)
                high = jnp.where(edge_lane < slots, above, mid)
                found[xi, py, 2] = pltpu.roll(high, lanes - slots, 1)
        return found

    for q, state in enumerate((ostate, vstate)):
        found = columns(
            lambda yl: osend[yl, q], lambda s, yl: orecv[s, yl, q], lambda d, at: oedges[slot_of[d], at, q]
        )
        for (xi, py, dz), value in found.items():
            state[xi, py, dz] = value

    lane_id = lax.broadcasted_iota(jnp.int32, (slots, lanes), 1)
    slot_id = lax.broadcasted_iota(jnp.int32, (slots, lanes), 0)
    pick = (lane_id // slots) * slots + slot_id
    itself = lax.rem(lane_id, slots) == slot_id

    def nearby(py, _):
        for px, (a, xl) in enumerate(px_of):
            for dz in range(3):
                block = ostate[xs.index(a), py, dz]
                for c in range(3):
                    r = c * nx + xl
                    row = jnp.broadcast_to(block[r : r + 1], (slots, lanes))
                    near[px, py, dz, c] = jnp.take_along_axis(row, pick, axis=1, mode="promise_in_bounds")
        return 0

    def out_planes(block, ref, y, mask):
        at = lax.broadcasted_iota(jnp.int32, (nz, lanes), 0) * slots + lax.rem(lane, slots)
        for x in range(nx):
            for c in range(3):
                r = c * nx + x
                row = jnp.broadcast_to(block[r : r + 1], (nz, lanes))
                plane = jnp.take_along_axis(row, at, axis=1, mode="promise_in_bounds")[:, :slots]
                if mask:
                    plane = jnp.where(occ_in[x, y] > 0, plane, o_in[x, y, c])
                ref[x, y, c] = plane

    half = 0.5 * TIME_STEP

    def step(k, _):
        p = lax.rem(k, 2)
        for py in range(ny + 2):
            nearby(py, 0)

        energy_rows = jnp.zeros((1, lanes), jnp.float32)
        for x in range(nx):
            def one_row(y, carried):
                block = ostate[0, y + 1, 1]
                mine = [block[c * nx + x : c * nx + x + 1] for c in range(3)]
                occupied = mine[0] < 0.5 * FAR
                force = [jnp.zeros((slots, lanes), jnp.float32) for _ in range(3)]
                energy = jnp.zeros((slots, lanes), jnp.float32)
                for dx in (-1, 0, 1):
                    for dy in (-1, 0, 1):
                        for dz in (-1, 0, 1):
                            shift = (dx, dy, dz)
                            apart = [
                                near[x + 1 + dx, y + 1 + dy, dz + 1, c] - (mine[c] - shift[c] * CELL_SIDE)
                                for c in range(3)
                            ]
                            squared = apart[0] * apart[0] + apart[1] * apart[1] + apart[2] * apart[2]
                            if shift == (0, 0, 0):
                                squared = jnp.where(itself, FAR, squared)
                            inside = squared < CUTOFF * CUTOFF
                            inv = lax.rsqrt(squared)
                            inv2 = inv * inv
                            inv6 = inv2 * inv2 * inv2
                            pull = inv * (FORCE_EDGE - inv * inv6 * (48.0 * inv6 - 24.0))
                            pull = jnp.where(inside, pull, 0.0)
                            for c in range(3):
                                force[c] = force[c] + pull * apart[c]
                            bond = inv6 * (4.0 * inv6 - 4.0) + (
                                squared * inv * FORCE_EDGE - (ENERGY_EDGE + CUTOFF * FORCE_EDGE)
                            )
                            energy = energy + jnp.where(inside, bond, 0.0)
                for c in range(3):
                    total = jnp.sum(force[c], axis=0, keepdims=True)
                    fsend[p, y, c * nx + x : c * nx + x + 1] = jnp.where(occupied, total, 0.0)
                total = jnp.sum(energy, axis=0, keepdims=True)
                return carried + jnp.where(occupied, total, 0.0)

            energy_rows = lax.fori_loop(0, ny, one_row, energy_rows)

        kinetic = jnp.zeros((tile, lanes), jnp.float32)
        for y in range(ny):
            v = vstate[0, y + 1, 1] + half * jnp.where(tile_row < 3 * nx, fsend[p, y], 0.0)
            kinetic = kinetic + v * v
        kinetic = 0.5 * jnp.sum(kinetic, keepdims=True)
        kinetic = jnp.broadcast_to(kinetic, (1, lanes))
        potential = jnp.broadcast_to(0.5 * jnp.sum(energy_rows, keepdims=True), (1, lanes))
        potential = jnp.where(lax.rem(lane[:1], slots) < slots // 2, potential, tally[...])
        numbers = jnp.where(lane[:1] < (tile - 1) * slots, kinetic, potential)
        fedges[p, my_id, 0] = numbers
        for y in range(ny):
            fsend[p, y, tile - 2 : tile - 1] = kinetic
            fsend[p, y, tile - 1 : tile] = potential
        for side in range(2):
            for y in range(ny):
                fedge[p, side, y] = packed(fsend[p, y], side)

        halo, distant = copies_of(
            fsend.at[p], frecv.at[p], fedge.at[p], lambda d, n: fedges.at[p, my_id, pl.ds(0, n)],
            f_send_sem, f_recv_sem.at[p], True,
        )
        @pl.when(k > 0)
        def _():
            for copy in distant:
                copy.start()

        for copy in halo:
            copy.start()

        @pl.when(k == STEPS)
        def _():
            for y in range(ny):
                out_planes(ostate[0, y + 1, 1], o_out, y, True)
                out_planes(fsend[p, y], f_out, y, False)

        for copy in halo:
            copy.wait()

        @pl.when(k > 0)
        def _():
            for copy in distant:
                copy.wait()

        for d in partners:
            if d[2] == 0:
                block = frecv[p, level_slot[d], layers_of(d[1])[0]]
                fedges[p, id_of(d), 0] = jnp.where(
                    lane[:1] < (tile - 1) * slots, block[tile - 2 : tile - 1], block[tile - 1 : tile]
                )
        parts = [fedges[p, d, 0] for d in range(devices)]
        while len(parts) > 1:
            parts = [sum(parts[i + 1 : i + 2], parts[i]) for i in range(0, len(parts), 2)]
        at = (tile - 2) * slots
        vigor = jnp.broadcast_to(parts[0][:, at : at + 1], (1, lanes))
        potential = jnp.broadcast_to(parts[0][:, lanes - slots : lanes - slots + 1], (1, lanes))
        count = jnp.broadcast_to(parts[0][:, lanes - 1 :], (1, lanes))
        warmth = 2.0 * vigor / (3.0 * count)
        lam = jnp.where(k == 0, 1.0, jnp.sqrt(1.0 + BATH_STRENGTH * (GOAL_WARMTH / warmth - 1.0)))
        which = lax.broadcasted_iota(jnp.int32, (2, lanes), 1)
        record = jnp.concatenate([potential, lam * lam * vigor], axis=0) / slot_total
        history[...] = jnp.where(which == k - 1, record, history[...])
        before = jnp.where(k > 0, half, 0.0)

        @pl.when(k < STEPS)
        def _():
            found = columns(
                lambda yl: fsend[p, yl], lambda s, yl: frecv[p, s, yl],
                lambda d, at: fedges[p, id_of(d), at],
            )
            for (xi, py, dz), f in found.items():
                f = jnp.where(tile_row < 3 * nx, f, 0.0)
                v = (vstate[xi, py, dz] + before * f) * lam
                v = v + half * f
                vstate[xi, py, dz] = v
                ostate[xi, py, dz] = ostate[xi, py, dz] + TIME_STEP * v

        @pl.when(k == STEPS)
        def _():
            for y in range(ny):
                v = (vstate[0, y + 1, 1] + half * fsend[p, y]) * lam
                out_planes(v, v_out, y, False)
            h_out[...] = history[:, :STEPS]

        return 0

    history[...] = jnp.zeros_like(history)
    lax.fori_loop(0, STEPS + 1, step, 0)


def shards(axes, offsets, velocities, occupied):
    gx, gy, gz = axes
    nx, ny, nz, slots = occupied.shape
    lanes = nz * slots
    tile = lanes // slots
    assert gz > 2 and tile >= 3 * nx + 2
    nxo, nyo, nzo = (len(offsets_of(s)) for s in axes)
    halo = nxo * nyo * nzo - 1
    level = nxo * nyo - 1
    devices = gx * gy * gz
    f32 = jnp.float32
    plane = jax.ShapeDtypeStruct((nx, ny, 3, nz, slots), f32)
    vmem = pl.BlockSpec(memory_space=pltpu.VMEM)
    dma = pltpu.SemaphoreType.DMA
    o, v, f, h = pl.pallas_call(
        functools.partial(kernel, axes, (nx, ny, nz, slots)),
        name="verlet",
        out_shape=[plane, plane, plane, jax.ShapeDtypeStruct((2, STEPS), f32)],
        in_specs=[vmem] * 3,
        out_specs=[vmem] * 4,
        scratch_shapes=[
            pltpu.VMEM((nxo, ny + 2, 3, tile, lanes), f32),
            pltpu.VMEM((nxo, ny + 2, 3, tile, lanes), f32),
            pltpu.VMEM((nx + 2, ny + 2, 3, 3, slots, lanes), f32),
            pltpu.VMEM((ny, 2, tile, lanes), f32),
            pltpu.VMEM((max(level, 1), ny, 2, tile, lanes), f32),
            pltpu.VMEM((2, ny, 2, 1, lanes), f32),
            pltpu.VMEM((halo, ny, 2, 1, lanes), f32),
            pltpu.VMEM((2, ny, tile, lanes), f32),
            pltpu.VMEM((2, max(level, 1), ny, tile, lanes), f32),
            pltpu.VMEM((2, 2, ny, 1, lanes), f32),
            pltpu.VMEM((2, devices, ny, 1, lanes), f32),
            pltpu.VMEM((1, lanes), f32),
            pltpu.VMEM((2, lanes), f32),
            dma((halo,)),
            dma((halo,)),
            dma((devices - 1,)),
            dma((2, devices - 1)),
        ],
        compiler_params=pltpu.CompilerParams(collective_id=0, has_side_effects=True),
    )(
        jnp.transpose(offsets, (0, 1, 4, 2, 3)),
        jnp.transpose(velocities, (0, 1, 4, 2, 3)),
        occupied,
    )
    back = (0, 1, 3, 4, 2)
    return (jnp.transpose(o, back), jnp.transpose(v, back), jnp.transpose(f, back), h.T)


def solution(mesh):
    axes = tuple(mesh.shape[a] for a in ("gx", "gy", "gz"))
    in_specs = (
        P("gx", "gy", "gz", None, None),
        P("gx", "gy", "gz", None, None),
        P("gx", "gy", "gz", None),
    )
    out_specs = (
        P("gx", "gy", "gz", None, None),
        P("gx", "gy", "gz", None, None),
        P("gx", "gy", "gz", None, None),
        P(),
    )
    return jax.shard_map(
        functools.partial(shards, axes), mesh=mesh, in_specs=in_specs, out_specs=out_specs, check_vma=False
    )
```

```python
import functools

import jax
import jax.numpy as jnp
from jax import lax
from jax.experimental import pallas as pl
from jax.experimental.pallas import tpu as pltpu
from jax.sharding import PartitionSpec as P

MESH = pl.DeviceIdType.MESH
STEPS = 4
CUTOFF = 2.5
CELL_SIDE = 2.6
TIME_STEP = 0.005
BATH_STRENGTH = 0.25
GOAL_WARMTH = 0.8
FORCE_EDGE = 24.0 * (2.0 * CUTOFF ** (-13) - CUTOFF ** (-7))
ENERGY_EDGE = 4.0 * (CUTOFF ** (-12) - CUTOFF ** (-6))
FAR = 1.0e15


def offsets_of(size):
    return [0] if size == 1 else [0, 1] if size == 2 else [0, 1, -1]


def kernel(
    axes, shape, o_in, v_in, occ_in, result,
    ostate, vstate, near, osend, orecv, oedge, oedges, fsend, frecv, fedge, fedges, tally, history,
    o_send_sem, o_recv_sem, f_send_sem, f_recv_sem,
):
    gx, gy, gz = axes
    nx, ny, nz, slots = shape
    lanes = nz * slots
    tile = fsend.shape[2]
    devices = gx * gy * gz
    slot_total = float(devices * nx * ny * lanes)
    me = [lax.axis_index(a) for a in ("gx", "gy", "gz")]
    my_id = (me[0] * gy + me[1]) * gz + me[2]

    turned = [[lax.rem(me[i] + j, n) for j in range(n)] for i, n in enumerate(axes)]

    def device(d):
        return tuple(turned[i][d[i] % axes[i]] for i in range(3))

    def id_of(d):
        at = device(d)
        return (at[0] * gy + at[1]) * gz + at[2]

    def canonical(size, off):
        return 0 if size == 1 else off % 2 if size == 2 else off

    def padded(size, n):
        return (
            [(canonical(size, -1), n - 1)]
            + [(0, i) for i in range(n)]
            + [(canonical(size, 1), 0)]
        )

    px_of, py_of = padded(gx, nx), padded(gy, ny)
    xs = offsets_of(gx)
    partners = [
        (a, b, c) for a in xs for b in offsets_of(gy) for c in offsets_of(gz) if (a, b, c) != (0, 0, 0)
    ]
    slot_of = {d: i for i, d in enumerate(partners)}
    met = {tuple(o % n for o, n in zip(d, axes)) for d in partners}
    far = [
        (a, b, c) for a in range(gx) for b in range(gy) for c in range(gz)
        if (a, b, c) not in met and (a, b, c) != (0, 0, 0)
    ]
    level_of = [i for i, d in enumerate(partners) if d[2] == 0]
    level_slot = {partners[i]: j for j, i in enumerate(level_of)}

    def layers_of(b):
        return sorted({yl for off, yl in py_of if off == b})

    def copies_of(send, recv, edge, edge_at, send_sem, recv_sem, with_far):
        copies, remote = [], []
        for i, d in enumerate(far if with_far else []):
            remote.append((edge.at[0, pl.ds(0, 1)], edge_at(d, 1), len(partners) + i, d))
        for i, d in reversed([*enumerate(partners)]):
            need = layers_of(d[1])
            where = pl.ds(need[0], len(need))
            if d[2] == 0:
                copies.append((send.at[where], recv.at[level_slot[d], where], i, d))
            else:
                copies.append((edge.at[0 if d[2] == 1 else 1, where], edge_at(d, len(need)), i, d))
        return [[
            pltpu.make_async_remote_copy(
                src_ref=src, dst_ref=dst, send_sem=send_sem.at[i], recv_sem=recv_sem.at[i],
                device_id=device(tuple(-x for x in d)), device_id_type=MESH,
            )
            for src, dst, i, d in chosen
        ] for chosen in ((copies, remote) if with_far else (copies,))]

    barrier = pltpu.get_barrier_semaphore()

    greeted = partners if max(n // 2 for n in axes) <= 3 else far + partners
    for d in greeted:
        pl.semaphore_signal(barrier, inc=1, device_id=device(d), device_id_type=MESH)

    lane = lax.broadcasted_iota(jnp.int32, (nz, lanes), 1)
    level = lax.broadcasted_iota(jnp.int32, (nz, lanes), 0)
    spread = (
        lax.rem(lax.broadcasted_iota(jnp.int32, (slots, lanes), 1), slots)
        == lax.broadcasted_iota(jnp.int32, (slots, lanes), 0)
    ).astype(jnp.float32)

    def rows_of(planes):
        flat = planes.reshape(-1, slots)
        wide = jnp.dot(flat, spread, precision=lax.Precision.HIGHEST, preferred_element_type=jnp.float32)
        wide = wide.reshape(-1, nz, lanes)
        return jnp.sum(jnp.where((lane // slots == level)[None], wide, 0.0), axis=1)

    o_rows = rows_of(o_in[...])
    v_rows = rows_of(v_in[...])
    w_rows = rows_of(occ_in[...].astype(jnp.float32))
    osend[...] = jnp.zeros_like(osend)
    fsend[...] = jnp.zeros_like(fsend)
    for x in range(nx):
        for y in range(ny):
            w = w_rows[x * ny + y : x * ny + y + 1]
            for c in range(3):
                i = (x * ny + y) * 3 + c
                r = c * nx + x
                osend[y, 0, r : r + 1] = jnp.where(w > 0.5, o_rows[i : i + 1], FAR)
                osend[y, 1, r : r + 1] = v_rows[i : i + 1] * w
    tally[...] = jnp.broadcast_to(jnp.sum(w_rows, keepdims=True), (1, lanes))

    tile_lane = lax.broadcasted_iota(jnp.int32, (tile, lanes), 1)
    tile_row = lax.broadcasted_iota(jnp.int32, (tile, lanes), 0)
    ends = [lax.rem(tile_lane, slots), lax.rem(tile_lane, slots) + (lanes - slots)]
    back = tile_row * slots + lax.rem(tile_lane, slots)

    def packed(block, side):
        taken = jnp.take_along_axis(block, ends[side], axis=1, mode="promise_in_bounds")
        return jnp.sum(jnp.where(tile_lane // slots == tile_row, taken, 0.0), axis=0, keepdims=True)

    def unpacked(row):
        wide = jnp.broadcast_to(row, (tile, lanes))
        return jnp.take_along_axis(wide, back, axis=1, mode="promise_in_bounds")

    for side in range(2):
        for y in range(ny):
            for q in range(2):
                oedge[side, y, q] = packed(osend[y, q], side)

    pl.semaphore_wait(barrier, len(greeted))
    (first,) = copies_of(
        osend, orecv, oedge, lambda d, n: oedges.at[slot_of[d], pl.ds(0, n)], o_send_sem, o_recv_sem, False
    )
    for copy in first:
        copy.start()
    for copy in first:
        copy.wait()

    edge_lane = tile_lane

    def columns(own, level_block, edge_row):
        found = {}
        for xi, a in enumerate(xs):
            for py, (b, yl) in enumerate(py_of):
                mid = own(yl) if (a, b) == (0, 0) else level_block(level_slot[a, b, 0], yl)
                found[xi, py, 1] = mid
                at = layers_of(b).index(yl)
                below, above = (unpacked(edge_row((a, b, c), at)) for c in (-1, 1))
                low = jnp.where(edge_lane >= lanes - slots, below, mid)
                found[xi, py, 0] = pltpu.roll(low, slots, 1)
                high = jnp.where(edge_lane < slots, above, mid)
                found[xi, py, 2] = pltpu.roll(high, lanes - slots, 1)
        return found

    for q, state in enumerate((ostate, vstate)):
        found = columns(
            lambda yl: osend[yl, q], lambda s, yl: orecv[s, yl, q], lambda d, at: oedges[slot_of[d], at, q]
        )
        for (xi, py, dz), value in found.items():
            state[xi, py, dz] = value

    lane_id = lax.broadcasted_iota(jnp.int32, (slots, lanes), 1)
    slot_id = lax.broadcasted_iota(jnp.int32, (slots, lanes), 0)
    pick = (lane_id // slots) * slots + slot_id
    itself = lax.rem(lane_id, slots) == slot_id

    def nearby(py, _):
        for px, (a, xl) in enumerate(px_of):
            for dz in range(3):
                block = ostate[xs.index(a), py, dz]
                for c in range(3):
                    r = c * nx + xl
                    row = jnp.broadcast_to(block[r : r + 1], (slots, lanes))
                    near[px, py, dz, c] = jnp.take_along_axis(row, pick, axis=1, mode="promise_in_bounds")
        return 0

    half = 0.5 * TIME_STEP

    def step(k, _):
        p = lax.rem(k, 2)
        for py in range(ny + 2):
            nearby(py, 0)

        energy_rows = jnp.zeros((1, lanes), jnp.float32)
        for x in range(nx):
            def one_row(y, carried):
                block = ostate[0, y + 1, 1]
                mine = [block[c * nx + x : c * nx + x + 1] for c in range(3)]
                occupied = mine[0] < 0.5 * FAR
                force = [jnp.zeros((slots, lanes), jnp.float32) for _ in range(3)]
                energy = jnp.zeros((slots, lanes), jnp.float32)
                for dx in (-1, 0, 1):
                    for dy in (-1, 0, 1):
                        for dz in (-1, 0, 1):
                            shift = (dx, dy, dz)
                            apart = [
                                near[x + 1 + dx, y + 1 + dy, dz + 1, c] - (mine[c] - shift[c] * CELL_SIDE)
                                for c in range(3)
                            ]
                            squared = apart[0] * apart[0] + apart[1] * apart[1] + apart[2] * apart[2]
                            if shift == (0, 0, 0):
                                squared = jnp.where(itself, FAR, squared)
                            inside = squared < CUTOFF * CUTOFF
                            inv = lax.rsqrt(squared)
                            inv2 = inv * inv
                            inv6 = inv2 * inv2 * inv2
                            pull = inv * (FORCE_EDGE - inv * inv6 * (48.0 * inv6 - 24.0))
                            pull = jnp.where(inside, pull, 0.0)
                            for c in range(3):
                                force[c] = force[c] + pull * apart[c]
                            bond = inv6 * (4.0 * inv6 - 4.0) + (
                                squared * inv * FORCE_EDGE - (ENERGY_EDGE + CUTOFF * FORCE_EDGE)
                            )
                            energy = energy + jnp.where(inside, bond, 0.0)
                for c in range(3):
                    total = jnp.sum(force[c], axis=0, keepdims=True)
                    fsend[p, y, c * nx + x : c * nx + x + 1] = jnp.where(occupied, total, 0.0)
                total = jnp.sum(energy, axis=0, keepdims=True)
                return carried + jnp.where(occupied, total, 0.0)

            energy_rows = lax.fori_loop(0, ny, one_row, energy_rows)

        kinetic = jnp.zeros((tile, lanes), jnp.float32)
        for y in range(ny):
            v = vstate[0, y + 1, 1] + half * jnp.where(tile_row < 3 * nx, fsend[p, y], 0.0)
            kinetic = kinetic + v * v
        kinetic = 0.5 * jnp.sum(kinetic, keepdims=True)
        kinetic = jnp.broadcast_to(kinetic, (1, lanes))
        potential = jnp.broadcast_to(0.5 * jnp.sum(energy_rows, keepdims=True), (1, lanes))
        potential = jnp.where(lax.rem(lane[:1], slots) < slots // 2, potential, tally[...])
        numbers = jnp.where(lane[:1] < (tile - 1) * slots, kinetic, potential)
        fedges[p, my_id, 0] = numbers
        for y in range(ny):
            fsend[p, y, tile - 2 : tile - 1] = kinetic
            fsend[p, y, tile - 1 : tile] = potential
        for side in range(2):
            for y in range(ny):
                fedge[p, side, y] = packed(fsend[p, y], side)

        halo, distant = copies_of(
            fsend.at[p], frecv.at[p], fedge.at[p], lambda d, n: fedges.at[p, my_id, pl.ds(0, n)],
            f_send_sem, f_recv_sem.at[p], True,
        )
        @pl.when(k > 0)
        def _():
            for copy in distant:
                copy.start()

        for copy in halo:
            copy.start()

        for copy in halo:
            copy.wait()

        @pl.when(k > 0)
        def _():
            for copy in distant:
                copy.wait()

        for d in partners:
            if d[2] == 0:
                block = frecv[p, level_slot[d], layers_of(d[1])[0]]
                fedges[p, id_of(d), 0] = jnp.where(
                    lane[:1] < (tile - 1) * slots, block[tile - 2 : tile - 1], block[tile - 1 : tile]
                )
        parts = [fedges[p, d, 0] for d in range(devices)]
        while len(parts) > 1:
            parts = [sum(parts[i + 1 : i + 2], parts[i]) for i in range(0, len(parts), 2)]
        at = (tile - 2) * slots
        vigor = jnp.broadcast_to(parts[0][:, at : at + 1], (1, lanes))
        potential = jnp.broadcast_to(parts[0][:, lanes - slots : lanes - slots + 1], (1, lanes))
        count = jnp.broadcast_to(parts[0][:, lanes - 1 :], (1, lanes))
        warmth = 2.0 * vigor / (3.0 * count)
        lam = jnp.where(k == 0, 1.0, jnp.sqrt(1.0 + BATH_STRENGTH * (GOAL_WARMTH / warmth - 1.0)))
        which = lax.broadcasted_iota(jnp.int32, (2, lanes), 1)
        record = jnp.concatenate([potential, lam * lam * vigor], axis=0) / slot_total
        history[...] = jnp.where(which == k - 1, record, history[...])
        before = jnp.where(k > 0, half, 0.0)

        @pl.when(k < STEPS)
        def _():
            found = columns(
                lambda yl: fsend[p, yl], lambda s, yl: frecv[p, s, yl],
                lambda d, at: fedges[p, id_of(d), at],
            )
            for (xi, py, dz), f in found.items():
                f = jnp.where(tile_row < 3 * nx, f, 0.0)
                v = (vstate[xi, py, dz] + before * f) * lam
                v = v + half * f
                vstate[xi, py, dz] = v
                ostate[xi, py, dz] = ostate[xi, py, dz] + TIME_STEP * v

        @pl.when(k == STEPS)
        def _():
            for y in range(ny):
                v = (vstate[0, y + 1, 1] + half * fsend[p, y]) * lam
                result[y] = ostate[0, y + 1, 1]
                result[ny + y] = v
                result[2 * ny + y] = fsend[p, y]
            result[3 * ny, 0:2] = history[...]

        return 0

    history[...] = jnp.zeros_like(history)
    lax.fori_loop(0, STEPS + 1, step, 0)


def unpack(shape, result, o_in, occ_in, o_out, v_out, f_out, h_out):
    nx, ny, nz, slots = shape
    lanes = nz * slots
    at = lax.broadcasted_iota(jnp.int32, (nz, lanes), 0) * slots + lax.rem(
        lax.broadcasted_iota(jnp.int32, (nz, lanes), 1), slots
    )
    for i, ref in enumerate((o_out, v_out, f_out)):
        for y in range(ny):
            for x in range(nx):
                for c in range(3):
                    r = c * nx + x
                    row = jnp.broadcast_to(result[i * ny + y, r : r + 1], (nz, lanes))
                    plane = jnp.take_along_axis(row, at, axis=1, mode="promise_in_bounds")[:, :slots]
                    if i == 0:
                        plane = jnp.where(occ_in[x, y] > 0, plane, o_in[x, y, c])
                    ref[x, y, c] = plane
    h_out[...] = result[3 * ny, 0:2, :STEPS]


def shards(axes, offsets, velocities, occupied):
    gx, gy, gz = axes
    nx, ny, nz, slots = occupied.shape
    lanes = nz * slots
    tile = lanes // slots
    assert gz > 2 and tile >= 3 * nx + 2
    nxo, nyo, nzo = (len(offsets_of(s)) for s in axes)
    halo = nxo * nyo * nzo - 1
    level = nxo * nyo - 1
    devices = gx * gy * gz
    f32 = jnp.float32
    plane = jax.ShapeDtypeStruct((nx, ny, 3, nz, slots), f32)
    vmem = pl.BlockSpec(memory_space=pltpu.VMEM)
    dma = pltpu.SemaphoreType.DMA
    o_planes = jnp.transpose(offsets, (0, 1, 4, 2, 3))
    result = pl.pallas_call(
        functools.partial(kernel, axes, (nx, ny, nz, slots)),
        name="verlet",
        out_shape=jax.ShapeDtypeStruct((3 * ny + 1, tile, lanes), f32),
        in_specs=[vmem] * 3,
        out_specs=vmem,
        scratch_shapes=[
            pltpu.VMEM((nxo, ny + 2, 3, tile, lanes), f32),
            pltpu.VMEM((nxo, ny + 2, 3, tile, lanes), f32),
            pltpu.VMEM((nx + 2, ny + 2, 3, 3, slots, lanes), f32),
            pltpu.VMEM((ny, 2, tile, lanes), f32),
            pltpu.VMEM((max(level, 1), ny, 2, tile, lanes), f32),
            pltpu.VMEM((2, ny, 2, 1, lanes), f32),
            pltpu.VMEM((halo, ny, 2, 1, lanes), f32),
            pltpu.VMEM((2, ny, tile, lanes), f32),
            pltpu.VMEM((2, max(level, 1), ny, tile, lanes), f32),
            pltpu.VMEM((2, 2, ny, 1, lanes), f32),
            pltpu.VMEM((2, devices, ny, 1, lanes), f32),
            pltpu.VMEM((1, lanes), f32),
            pltpu.VMEM((2, lanes), f32),
            dma((halo,)),
            dma((halo,)),
            dma((devices - 1,)),
            dma((2, devices - 1)),
        ],
        compiler_params=pltpu.CompilerParams(collective_id=0, has_side_effects=True),
    )(
        o_planes,
        jnp.transpose(velocities, (0, 1, 4, 2, 3)),
        occupied,
    )
    o, v, f, h = pl.pallas_call(
        functools.partial(unpack, (nx, ny, nz, slots)),
        name="unpack",
        out_shape=[plane, plane, plane, jax.ShapeDtypeStruct((2, STEPS), f32)],
        in_specs=[vmem] * 3,
        out_specs=[vmem] * 4,
    )(result, o_planes, occupied)
    back = (0, 1, 3, 4, 2)
    return (jnp.transpose(o, back), jnp.transpose(v, back), jnp.transpose(f, back), h.T)


def solution(mesh):
    axes = tuple(mesh.shape[a] for a in ("gx", "gy", "gz"))
    in_specs = (
        P("gx", "gy", "gz", None, None),
        P("gx", "gy", "gz", None, None),
        P("gx", "gy", "gz", None),
    )
    out_specs = (
        P("gx", "gy", "gz", None, None),
        P("gx", "gy", "gz", None, None),
        P("gx", "gy", "gz", None, None),
        P(),
    )
    return jax.shard_map(
        functools.partial(shards, axes), mesh=mesh, in_specs=in_specs, out_specs=out_specs, check_vma=False
    )
```

```python
import functools

import jax
import jax.numpy as jnp
from jax import lax
from jax.experimental import pallas as pl
from jax.experimental.pallas import tpu as pltpu
from jax.sharding import PartitionSpec as P

MESH = pl.DeviceIdType.MESH
STEPS = 4
CUTOFF = 2.5
CELL_SIDE = 2.6
TIME_STEP = 0.005
BATH_STRENGTH = 0.25
GOAL_WARMTH = 0.8
FORCE_EDGE = 24.0 * (2.0 * CUTOFF ** (-13) - CUTOFF ** (-7))
ENERGY_EDGE = 4.0 * (CUTOFF ** (-12) - CUTOFF ** (-6))
FAR = 1.0e15


def offsets_of(size):
    return [0] if size == 1 else [0, 1] if size == 2 else [0, 1, -1]


def kernel(
    axes, shape, o_in, v_in, occ_in, result,
    ostate, vstate, near, osend, orecv, oedge, oedges, fsend, frecv, fedge, fedges, tally, history,
    o_send_sem, o_recv_sem, f_send_sem, f_recv_sem,
):
    gx, gy, gz = axes
    nx, ny, nz, slots = shape
    lanes = nz * slots
    tile = fsend.shape[2]
    devices = gx * gy * gz
    slot_total = float(devices * nx * ny * lanes)
    me = [lax.axis_index(a) for a in ("gx", "gy", "gz")]
    my_id = (me[0] * gy + me[1]) * gz + me[2]

    turned = [[lax.rem(me[i] + j, n) for j in range(n)] for i, n in enumerate(axes)]

    def device(d):
        return tuple(turned[i][d[i] % axes[i]] for i in range(3))

    def id_of(d):
        at = device(d)
        return (at[0] * gy + at[1]) * gz + at[2]

    def canonical(size, off):
        return 0 if size == 1 else off % 2 if size == 2 else off

    def padded(size, n):
        return (
            [(canonical(size, -1), n - 1)]
            + [(0, i) for i in range(n)]
            + [(canonical(size, 1), 0)]
        )

    px_of, py_of = padded(gx, nx), padded(gy, ny)
    xs = offsets_of(gx)
    partners = [
        (a, b, c) for a in xs for b in offsets_of(gy) for c in offsets_of(gz) if (a, b, c) != (0, 0, 0)
    ]
    slot_of = {d: i for i, d in enumerate(partners)}
    met = {tuple(o % n for o, n in zip(d, axes)) for d in partners}
    far = [
        (a, b, c) for a in range(gx) for b in range(gy) for c in range(gz)
        if (a, b, c) not in met and (a, b, c) != (0, 0, 0)
    ]
    level_of = [i for i, d in enumerate(partners) if d[2] == 0]
    level_slot = {partners[i]: j for j, i in enumerate(level_of)}

    def layers_of(b):
        return sorted({yl for off, yl in py_of if off == b})

    def copies_of(send, recv, edge, edge_at, send_sem, recv_sem, with_far):
        copies, remote = [], []
        for i, d in enumerate(far if with_far else []):
            remote.append((edge.at[0, pl.ds(0, 1)], edge_at(d, 1), len(partners) + i, d))
        for i, d in reversed([*enumerate(partners)]):
            need = layers_of(d[1])
            where = pl.ds(need[0], len(need))
            if d[2] == 0:
                copies.append((send.at[where], recv.at[level_slot[d], where], i, d))
            else:
                copies.append((edge.at[0 if d[2] == 1 else 1, where], edge_at(d, len(need)), i, d))
        return [[
            pltpu.make_async_remote_copy(
                src_ref=src, dst_ref=dst, send_sem=send_sem.at[i], recv_sem=recv_sem.at[i],
                device_id=device(tuple(-x for x in d)), device_id_type=MESH,
            )
            for src, dst, i, d in chosen
        ] for chosen in ((copies, remote) if with_far else (copies,))]

    barrier = pltpu.get_barrier_semaphore()

    greeted = partners if max(n // 2 for n in axes) <= 3 else far + partners
    for d in greeted:
        pl.semaphore_signal(barrier, inc=1, device_id=device(d), device_id_type=MESH)

    lane = lax.broadcasted_iota(jnp.int32, (nz, lanes), 1)
    level = lax.broadcasted_iota(jnp.int32, (nz, lanes), 0)
    spread = (
        lax.rem(lax.broadcasted_iota(jnp.int32, (slots, lanes), 1), slots)
        == lax.broadcasted_iota(jnp.int32, (slots, lanes), 0)
    ).astype(jnp.float32)

    def rows_of(planes):
        flat = planes.reshape(-1, slots)
        wide = jnp.dot(flat, spread, precision=lax.Precision.HIGHEST, preferred_element_type=jnp.float32)
        wide = wide.reshape(-1, nz, lanes)
        return jnp.sum(jnp.where((lane // slots == level)[None], wide, 0.0), axis=1)

    o_rows = rows_of(o_in[...])
    v_rows = rows_of(v_in[...])
    w_rows = rows_of(occ_in[...].astype(jnp.float32))
    osend[...] = jnp.zeros_like(osend)
    fsend[...] = jnp.zeros_like(fsend)
    for x in range(nx):
        for y in range(ny):
            w = w_rows[x * ny + y : x * ny + y + 1]
            for c in range(3):
                i = (x * ny + y) * 3 + c
                r = c * nx + x
                osend[y, 0, r : r + 1] = jnp.where(w > 0.5, o_rows[i : i + 1], FAR)
                osend[y, 1, r : r + 1] = v_rows[i : i + 1] * w
    tally[...] = jnp.broadcast_to(jnp.sum(w_rows, keepdims=True), (1, lanes))

    tile_lane = lax.broadcasted_iota(jnp.int32, (tile, lanes), 1)
    tile_row = lax.broadcasted_iota(jnp.int32, (tile, lanes), 0)
    ends = [lax.rem(tile_lane, slots), lax.rem(tile_lane, slots) + (lanes - slots)]
    back = tile_row * slots + lax.rem(tile_lane, slots)

    def packed(block, side):
        taken = jnp.take_along_axis(block, ends[side], axis=1, mode="promise_in_bounds")
        return jnp.sum(jnp.where(tile_lane // slots == tile_row, taken, 0.0), axis=0, keepdims=True)

    def unpacked(row):
        wide = jnp.broadcast_to(row, (tile, lanes))
        return jnp.take_along_axis(wide, back, axis=1, mode="promise_in_bounds")

    for side in range(2):
        for y in range(ny):
            for q in range(2):
                oedge[side, y, q] = packed(osend[y, q], side)

    pl.semaphore_wait(barrier, len(greeted))
    (first,) = copies_of(
        osend, orecv, oedge, lambda d, n: oedges.at[slot_of[d], pl.ds(0, n)], o_send_sem, o_recv_sem, False
    )
    for copy in first:
        copy.start()
    for copy in first:
        copy.wait()

    edge_lane = tile_lane

    def columns(own, level_block, edge_row):
        found = {}
        for xi, a in enumerate(xs):
            for py, (b, yl) in enumerate(py_of):
                mid = own(yl) if (a, b) == (0, 0) else level_block(level_slot[a, b, 0], yl)
                found[xi, py, 1] = mid
                at = layers_of(b).index(yl)
                below, above = (unpacked(edge_row((a, b, c), at)) for c in (-1, 1))
                low = jnp.where(edge_lane >= lanes - slots, below, mid)
                found[xi, py, 0] = pltpu.roll(low, slots, 1)
                high = jnp.where(edge_lane < slots, above, mid)
                found[xi, py, 2] = pltpu.roll(high, lanes - slots, 1)
        return found

    for q, state in enumerate((ostate, vstate)):
        found = columns(
            lambda yl: osend[yl, q], lambda s, yl: orecv[s, yl, q], lambda d, at: oedges[slot_of[d], at, q]
        )
        for (xi, py, dz), value in found.items():
            state[xi, py, dz] = value

    lane_id = lax.broadcasted_iota(jnp.int32, (slots, lanes), 1)
    slot_id = lax.broadcasted_iota(jnp.int32, (slots, lanes), 0)
    pick = (lane_id // slots) * slots + slot_id
    itself = lax.rem(lane_id, slots) == slot_id

    def nearby(py, _):
        for px, (a, xl) in enumerate(px_of):
            for dz in range(3):
                for c in range(3):
                    r = c * nx + xl
                    row = jnp.broadcast_to(ostate[xs.index(a), py, dz, r : r + 1], (slots, lanes))
                    near[px, py, dz, c] = jnp.take_along_axis(row, pick, axis=1, mode="promise_in_bounds")
        return 0

    half = 0.5 * TIME_STEP

    def step(k, _):
        p = lax.rem(k, 2)
        for py in range(ny + 2):
            nearby(py, 0)

        energy_rows = jnp.zeros((1, lanes), jnp.float32)
        for x in range(nx):
            def one_row(y, carried):
                block = ostate[0, y + 1, 1]
                mine = [block[c * nx + x : c * nx + x + 1] for c in range(3)]
                occupied = mine[0] < 0.5 * FAR
                force = [jnp.zeros((slots, lanes), jnp.float32) for _ in range(3)]
                bonds, reach, pairs = (jnp.zeros((slots, lanes), jnp.float32) for _ in range(3))
                for dx in (-1, 0, 1):
                    for dy in (-1, 0, 1):
                        for dz in (-1, 0, 1):
                            shift = (dx, dy, dz)
                            apart = [
                                near[x + 1 + dx, y + 1 + dy, dz + 1, c] - (mine[c] - shift[c] * CELL_SIDE)
                                for c in range(3)
                            ]
                            squared = apart[0] * apart[0] + apart[1] * apart[1] + apart[2] * apart[2]
                            if shift == (0, 0, 0):
                                squared = jnp.where(itself, FAR, squared)
                            inside = squared < CUTOFF * CUTOFF
                            inv = jnp.where(inside, lax.rsqrt(squared), 0.0)
                            inv2 = inv * inv
                            inv6 = inv2 * inv2 * inv2
                            less = inv6 - 1.0
                            pull = inv * (FORCE_EDGE / 24.0 - inv * inv6 * (inv6 + less))
                            for c in range(3):
                                force[c] = force[c] + pull * apart[c]
                            bonds = bonds + inv6 * less
                            reach = reach + squared * inv
                            pairs = pairs + jnp.where(inside, 1.0, 0.0)
                for c in range(3):
                    total = 24.0 * jnp.sum(force[c], axis=0, keepdims=True)
                    fsend[p, y, c * nx + x : c * nx + x + 1] = jnp.where(occupied, total, 0.0)
                energy = 4.0 * bonds + FORCE_EDGE * reach - (ENERGY_EDGE + CUTOFF * FORCE_EDGE) * pairs
                total = jnp.sum(energy, axis=0, keepdims=True)
                return carried + jnp.where(occupied, total, 0.0)

            energy_rows = lax.fori_loop(0, ny, one_row, energy_rows)

        kinetic = jnp.zeros((tile, lanes), jnp.float32)
        for y in range(ny):
            v = vstate[0, y + 1, 1] + half * jnp.where(tile_row < 3 * nx, fsend[p, y], 0.0)
            kinetic = kinetic + v * v
        kinetic = 0.5 * jnp.sum(kinetic, keepdims=True)
        kinetic = jnp.broadcast_to(kinetic, (1, lanes))
        potential = jnp.broadcast_to(0.5 * jnp.sum(energy_rows, keepdims=True), (1, lanes))
        potential = jnp.where(lax.rem(lane[:1], slots) < slots // 2, potential, tally[...])
        numbers = jnp.where(lane[:1] < (tile - 1) * slots, kinetic, potential)
        fedges[p, my_id, 0] = numbers
        for y in range(ny):
            fsend[p, y, tile - 2 : tile - 1] = kinetic
            fsend[p, y, tile - 1 : tile] = potential
        for side in range(2):
            for y in range(ny):
                fedge[p, side, y] = packed(fsend[p, y], side)

        halo, distant = copies_of(
            fsend.at[p], frecv.at[p], fedge.at[p], lambda d, n: fedges.at[p, my_id, pl.ds(0, n)],
            f_send_sem, f_recv_sem.at[p], True,
        )
        @pl.when(k > 0)
        def _():
            for copy in distant:
                copy.start()

        for copy in halo:
            copy.start()

        for copy in halo:
            copy.wait()

        @pl.when(k > 0)
        def _():
            for copy in distant:
                copy.wait()

        for d in partners:
            if d[2] == 0:
                block = frecv[p, level_slot[d], layers_of(d[1])[0]]
                fedges[p, id_of(d), 0] = jnp.where(
                    lane[:1] < (tile - 1) * slots, block[tile - 2 : tile - 1], block[tile - 1 : tile]
                )
        parts = [fedges[p, d, 0] for d in range(devices)]
        while len(parts) > 1:
            parts = [sum(parts[i + 1 : i + 2], parts[i]) for i in range(0, len(parts), 2)]
        at = (tile - 2) * slots
        vigor = jnp.broadcast_to(parts[0][:, at : at + 1], (1, lanes))
        potential = jnp.broadcast_to(parts[0][:, lanes - slots : lanes - slots + 1], (1, lanes))
        count = jnp.broadcast_to(parts[0][:, lanes - 1 :], (1, lanes))
        warmth = 2.0 * vigor / (3.0 * count)
        lam = jnp.where(k == 0, 1.0, jnp.sqrt(1.0 + BATH_STRENGTH * (GOAL_WARMTH / warmth - 1.0)))
        which = lax.broadcasted_iota(jnp.int32, (2, lanes), 1)
        record = jnp.concatenate([potential, lam * lam * vigor], axis=0) / slot_total
        history[...] = jnp.where(which == k - 1, record, history[...])
        before = jnp.where(k > 0, half, 0.0)

        @pl.when(k < STEPS)
        def _():
            found = columns(
                lambda yl: fsend[p, yl], lambda s, yl: frecv[p, s, yl],
                lambda d, at: fedges[p, id_of(d), at],
            )
            for (xi, py, dz), f in found.items():
                f = jnp.where(tile_row < 3 * nx, f, 0.0)
                v = (vstate[xi, py, dz] + before * f) * lam
                v = v + half * f
                vstate[xi, py, dz] = v
                ostate[xi, py, dz] = ostate[xi, py, dz] + TIME_STEP * v

        @pl.when(k == STEPS)
        def _():
            for y in range(ny):
                v = (vstate[0, y + 1, 1] + half * fsend[p, y]) * lam
                result[y] = ostate[0, y + 1, 1]
                result[ny + y] = v
                result[2 * ny + y] = fsend[p, y]
            result[3 * ny, 0:2] = history[...]

        return 0

    history[...] = jnp.zeros_like(history)
    lax.fori_loop(0, STEPS + 1, step, 0)


def unpack(shape, result, o_in, occ_in, o_out, v_out, f_out, h_out):
    nx, ny, nz, slots = shape
    lanes = nz * slots
    at = lax.broadcasted_iota(jnp.int32, (nz, lanes), 0) * slots + lax.rem(
        lax.broadcasted_iota(jnp.int32, (nz, lanes), 1), slots
    )
    for i, ref in enumerate((o_out, v_out, f_out)):
        for y in range(ny):
            for x in range(nx):
                for c in range(3):
                    r = c * nx + x
                    row = jnp.broadcast_to(result[i * ny + y, r : r + 1], (nz, lanes))
                    plane = jnp.take_along_axis(row, at, axis=1, mode="promise_in_bounds")[:, :slots]
                    if i == 0:
                        plane = jnp.where(occ_in[x, y] > 0, plane, o_in[x, y, c])
                    ref[x, y, c] = plane
    h_out[...] = result[3 * ny, 0:2, :STEPS]


def shards(axes, offsets, velocities, occupied):
    gx, gy, gz = axes
    nx, ny, nz, slots = occupied.shape
    lanes = nz * slots
    tile = lanes // slots
    assert gz > 2 and tile >= 3 * nx + 2
    nxo, nyo, nzo = (len(offsets_of(s)) for s in axes)
    halo = nxo * nyo * nzo - 1
    level = nxo * nyo - 1
    devices = gx * gy * gz
    f32 = jnp.float32
    plane = jax.ShapeDtypeStruct((nx, ny, 3, nz, slots), f32)
    vmem = pl.BlockSpec(memory_space=pltpu.VMEM)
    dma = pltpu.SemaphoreType.DMA
    o_planes = jnp.transpose(offsets, (0, 1, 4, 2, 3))
    result = pl.pallas_call(
        functools.partial(kernel, axes, (nx, ny, nz, slots)),
        name="verlet",
        out_shape=jax.ShapeDtypeStruct((3 * ny + 1, tile, lanes), f32),
        in_specs=[vmem] * 3,
        out_specs=vmem,
        scratch_shapes=[
            pltpu.VMEM((nxo, ny + 2, 3, tile, lanes), f32),
            pltpu.VMEM((nxo, ny + 2, 3, tile, lanes), f32),
            pltpu.VMEM((nx + 2, ny + 2, 3, 3, slots, lanes), f32),
            pltpu.VMEM((ny, 2, tile, lanes), f32),
            pltpu.VMEM((max(level, 1), ny, 2, tile, lanes), f32),
            pltpu.VMEM((2, ny, 2, 1, lanes), f32),
            pltpu.VMEM((halo, ny, 2, 1, lanes), f32),
            pltpu.VMEM((2, ny, tile, lanes), f32),
            pltpu.VMEM((2, max(level, 1), ny, tile, lanes), f32),
            pltpu.VMEM((2, 2, ny, 1, lanes), f32),
            pltpu.VMEM((2, devices, ny, 1, lanes), f32),
            pltpu.VMEM((1, lanes), f32),
            pltpu.VMEM((2, lanes), f32),
            dma((halo,)),
            dma((halo,)),
            dma((devices - 1,)),
            dma((2, devices - 1)),
        ],
        compiler_params=pltpu.CompilerParams(collective_id=0, has_side_effects=True),
    )(
        o_planes,
        jnp.transpose(velocities, (0, 1, 4, 2, 3)),
        occupied,
    )
    o, v, f, h = pl.pallas_call(
        functools.partial(unpack, (nx, ny, nz, slots)),
        name="unpack",
        out_shape=[plane, plane, plane, jax.ShapeDtypeStruct((2, STEPS), f32)],
        in_specs=[vmem] * 3,
        out_specs=[vmem] * 4,
    )(result, o_planes, occupied)
    back = (0, 1, 3, 4, 2)
    return (jnp.transpose(o, back), jnp.transpose(v, back), jnp.transpose(f, back), h.T)


def solution(mesh):
    axes = tuple(mesh.shape[a] for a in ("gx", "gy", "gz"))
    in_specs = (
        P("gx", "gy", "gz", None, None),
        P("gx", "gy", "gz", None, None),
        P("gx", "gy", "gz", None),
    )
    out_specs = (
        P("gx", "gy", "gz", None, None),
        P("gx", "gy", "gz", None, None),
        P("gx", "gy", "gz", None, None),
        P(),
    )
    return jax.shard_map(
        functools.partial(shards, axes), mesh=mesh, in_specs=in_specs, out_specs=out_specs, check_vma=False
    )
```

```python
import functools

import jax
import jax.numpy as jnp
from jax import lax
from jax.experimental import pallas as pl
from jax.experimental.pallas import tpu as pltpu
from jax.sharding import PartitionSpec as P

MESH = pl.DeviceIdType.MESH
STEPS = 4
CUTOFF = 2.5
CELL_SIDE = 2.6
TIME_STEP = 0.005
BATH_STRENGTH = 0.25
GOAL_WARMTH = 0.8
FORCE_EDGE = 24.0 * (2.0 * CUTOFF ** (-13) - CUTOFF ** (-7))
ENERGY_EDGE = 4.0 * (CUTOFF ** (-12) - CUTOFF ** (-6))
FAR = 1.0e15


def offsets_of(size):
    return [0] if size == 1 else [0, 1] if size == 2 else [0, 1, -1]


def kernel(
    axes, shape, o_in, v_in, occ_in, result,
    ostate, vstate, near, osend, orecv, oedge, oedges, fsend, frecv, fedge, fedges, tally, history,
    o_send_sem, o_recv_sem, f_send_sem, f_recv_sem,
):
    gx, gy, gz = axes
    nx, ny, nz, slots = shape
    lanes = nz * slots
    tile = fsend.shape[2]
    devices = gx * gy * gz
    slot_total = float(devices * nx * ny * lanes)
    me = [lax.axis_index(a) for a in ("gx", "gy", "gz")]
    my_id = (me[0] * gy + me[1]) * gz + me[2]

    turned = [[lax.rem(me[i] + j, n) for j in range(n)] for i, n in enumerate(axes)]

    def device(d):
        return tuple(turned[i][d[i] % axes[i]] for i in range(3))

    def id_of(d):
        at = device(d)
        return (at[0] * gy + at[1]) * gz + at[2]

    def canonical(size, off):
        return 0 if size == 1 else off % 2 if size == 2 else off

    def padded(size, n):
        return (
            [(canonical(size, -1), n - 1)]
            + [(0, i) for i in range(n)]
            + [(canonical(size, 1), 0)]
        )

    px_of, py_of = padded(gx, nx), padded(gy, ny)
    xs = offsets_of(gx)
    partners = [
        (a, b, c) for a in xs for b in offsets_of(gy) for c in offsets_of(gz) if (a, b, c) != (0, 0, 0)
    ]
    slot_of = {d: i for i, d in enumerate(partners)}
    met = {tuple(o % n for o, n in zip(d, axes)) for d in partners}
    far = [
        (a, b, c) for a in range(gx) for b in range(gy) for c in range(gz)
        if (a, b, c) not in met and (a, b, c) != (0, 0, 0)
    ]
    level_of = [i for i, d in enumerate(partners) if d[2] == 0]
    level_slot = {partners[i]: j for j, i in enumerate(level_of)}

    def layers_of(b):
        return sorted({yl for off, yl in py_of if off == b})

    def copies_of(send, recv, edge, edge_at, send_sem, recv_sem, with_far):
        copies, remote = [], []
        for i, d in enumerate(far if with_far else []):
            remote.append((edge.at[0, pl.ds(0, 1)], edge_at(d, 1), len(partners) + i, d))
        for i, d in reversed([*enumerate(partners)]):
            need = layers_of(d[1])
            where = pl.ds(need[0], len(need))
            if d[2] == 0:
                copies.append((send.at[where], recv.at[level_slot[d], where], i, d))
            else:
                copies.append((edge.at[0 if d[2] == 1 else 1, where], edge_at(d, len(need)), i, d))
        return [[
            pltpu.make_async_remote_copy(
                src_ref=src, dst_ref=dst, send_sem=send_sem.at[i], recv_sem=recv_sem.at[i],
                device_id=device(tuple(-x for x in d)), device_id_type=MESH,
            )
            for src, dst, i, d in chosen
        ] for chosen in ((copies, remote) if with_far else (copies,))]

    barrier = pltpu.get_barrier_semaphore()

    greeted = partners if max(n // 2 for n in axes) <= 3 else far + partners
    for d in greeted:
        pl.semaphore_signal(barrier, inc=1, device_id=device(d), device_id_type=MESH)

    lane = lax.broadcasted_iota(jnp.int32, (nz, lanes), 1)
    level = lax.broadcasted_iota(jnp.int32, (nz, lanes), 0)
    spread = (
        lax.rem(lax.broadcasted_iota(jnp.int32, (slots, lanes), 1), slots)
        == lax.broadcasted_iota(jnp.int32, (slots, lanes), 0)
    ).astype(jnp.float32)

    def rows_of(planes):
        flat = planes.reshape(-1, slots)
        wide = jnp.dot(flat, spread, precision=lax.Precision.HIGHEST, preferred_element_type=jnp.float32)
        wide = wide.reshape(-1, nz, lanes)
        return jnp.sum(jnp.where((lane // slots == level)[None], wide, 0.0), axis=1)

    o_rows = rows_of(o_in[...])
    v_rows = rows_of(v_in[...])
    w_rows = rows_of(occ_in[...].astype(jnp.float32))
    osend[...] = jnp.zeros_like(osend)
    fsend[...] = jnp.zeros_like(fsend)
    for x in range(nx):
        for y in range(ny):
            w = w_rows[x * ny + y : x * ny + y + 1]
            for c in range(3):
                i = (x * ny + y) * 3 + c
                r = c * nx + x
                osend[y, 0, r : r + 1] = jnp.where(w > 0.5, o_rows[i : i + 1], FAR)
                osend[y, 1, r : r + 1] = v_rows[i : i + 1] * w
    tally[...] = jnp.broadcast_to(jnp.sum(w_rows, keepdims=True), (1, lanes))

    tile_lane = lax.broadcasted_iota(jnp.int32, (tile, lanes), 1)
    tile_row = lax.broadcasted_iota(jnp.int32, (tile, lanes), 0)
    ends = [lax.rem(tile_lane, slots), lax.rem(tile_lane, slots) + (lanes - slots)]
    back = tile_row * slots + lax.rem(tile_lane, slots)

    def packed(block, side):
        taken = jnp.take_along_axis(block, ends[side], axis=1, mode="promise_in_bounds")
        return jnp.sum(jnp.where(tile_lane // slots == tile_row, taken, 0.0), axis=0, keepdims=True)

    def unpacked(row):
        wide = jnp.broadcast_to(row, (tile, lanes))
        return jnp.take_along_axis(wide, back, axis=1, mode="promise_in_bounds")

    for side in range(2):
        for y in range(ny):
            for q in range(2):
                oedge[side, y, q] = packed(osend[y, q], side)

    pl.semaphore_wait(barrier, len(greeted))
    (first,) = copies_of(
        osend, orecv, oedge, lambda d, n: oedges.at[slot_of[d], pl.ds(0, n)], o_send_sem, o_recv_sem, False
    )
    for copy in first:
        copy.start()
    for copy in first:
        copy.wait()

    edge_lane = tile_lane

    def columns(own, level_block, edge_row):
        found = {}
        for xi, a in enumerate(xs):
            for py, (b, yl) in enumerate(py_of):
                mid = own(yl) if (a, b) == (0, 0) else level_block(level_slot[a, b, 0], yl)
                found[xi, py, 1] = mid
                at = layers_of(b).index(yl)
                below, above = (unpacked(edge_row((a, b, c), at)) for c in (-1, 1))
                low = jnp.where(edge_lane >= lanes - slots, below, mid)
                found[xi, py, 0] = pltpu.roll(low, slots, 1)
                high = jnp.where(edge_lane < slots, above, mid)
                found[xi, py, 2] = pltpu.roll(high, lanes - slots, 1)
        return found

    for q, state in enumerate((ostate, vstate)):
        found = columns(
            lambda yl: osend[yl, q], lambda s, yl: orecv[s, yl, q], lambda d, at: oedges[slot_of[d], at, q]
        )
        for (xi, py, dz), value in found.items():
            state[xi, py, dz] = value

    lane_id = lax.broadcasted_iota(jnp.int32, (slots, lanes), 1)
    slot_id = lax.broadcasted_iota(jnp.int32, (slots, lanes), 0)
    pick = (lane_id // slots) * slots + slot_id
    itself = lax.rem(lane_id, slots) == slot_id

    def nearby(py, _):
        for px, (a, xl) in enumerate(px_of):
            for dz in range(3):
                for c in range(3):
                    r = c * nx + xl
                    row = jnp.broadcast_to(ostate[xs.index(a), py, dz, r : r + 1], (slots, lanes))
                    near[px, py, dz, c] = jnp.take_along_axis(row, pick, axis=1, mode="promise_in_bounds")
        return 0

    half = 0.5 * TIME_STEP

    def step(k, _):
        p = lax.rem(k, 2)
        for py in range(ny + 2):
            nearby(py, 0)

        energy_rows = jnp.zeros((1, lanes), jnp.float32)
        for x in range(nx):
            def one_row(y, carried):
                block = ostate[0, y + 1, 1]
                mine = [block[c * nx + x : c * nx + x + 1] for c in range(3)]
                occupied = mine[0] < 0.5 * FAR
                force = [jnp.zeros((slots, lanes), jnp.float32) for _ in range(3)]
                bonds, reach, pairs = (jnp.zeros((slots, lanes), jnp.float32) for _ in range(3))
                for dx in (-1, 0, 1):
                    for dy in (-1, 0, 1):
                        for dz in (-1, 0, 1):
                            shift = (dx, dy, dz)
                            apart = [
                                near[x + 1 + dx, y + 1 + dy, dz + 1, c] - (mine[c] - shift[c] * CELL_SIDE)
                                for c in range(3)
                            ]
                            squared = apart[0] * apart[0] + apart[1] * apart[1] + apart[2] * apart[2]
                            if shift == (0, 0, 0):
                                squared = jnp.where(itself, FAR, squared)
                            inside = squared < CUTOFF * CUTOFF
                            inv = jnp.where(inside, lax.rsqrt(squared), 0.0)
                            inv2 = inv * inv
                            inv6 = inv2 * inv2 * inv2
                            less = inv6 - 1.0
                            pull = inv * (FORCE_EDGE / 24.0 - inv * inv6 * (inv6 + less))
                            for c in range(3):
                                force[c] = force[c] + pull * apart[c]
                            bonds = bonds + inv6 * less
                            reach = reach + squared * inv
                            pairs = pairs + jnp.where(inside, 1.0, 0.0)
                for c in range(3):
                    total = 24.0 * jnp.sum(force[c], axis=0, keepdims=True)
                    fsend[p, y, c * nx + x : c * nx + x + 1] = jnp.where(occupied, total, 0.0)
                energy = 4.0 * bonds + FORCE_EDGE * reach - (ENERGY_EDGE + CUTOFF * FORCE_EDGE) * pairs
                total = jnp.sum(energy, axis=0, keepdims=True)
                return carried + jnp.where(occupied, total, 0.0)

            for y in range(ny):
                energy_rows = one_row(y, energy_rows)

        kinetic = jnp.zeros((tile, lanes), jnp.float32)
        for y in range(ny):
            v = vstate[0, y + 1, 1] + half * jnp.where(tile_row < 3 * nx, fsend[p, y], 0.0)
            kinetic = kinetic + v * v
        kinetic = 0.5 * jnp.sum(kinetic, keepdims=True)
        kinetic = jnp.broadcast_to(kinetic, (1, lanes))
        potential = jnp.broadcast_to(0.5 * jnp.sum(energy_rows, keepdims=True), (1, lanes))
        potential = jnp.where(lax.rem(lane[:1], slots) < slots // 2, potential, tally[...])
        numbers = jnp.where(lane[:1] < (tile - 1) * slots, kinetic, potential)
        fedges[p, my_id, 0] = numbers
        for y in range(ny):
            fsend[p, y, tile - 2 : tile - 1] = kinetic
            fsend[p, y, tile - 1 : tile] = potential
        for side in range(2):
            for y in range(ny):
                fedge[p, side, y] = packed(fsend[p, y], side)

        halo, distant = copies_of(
            fsend.at[p], frecv.at[p], fedge.at[p], lambda d, n: fedges.at[p, my_id, pl.ds(0, n)],
            f_send_sem, f_recv_sem.at[p], True,
        )
        @pl.when(k > 0)
        def _():
            for copy in distant:
                copy.start()

        for copy in halo:
            copy.start()

        for copy in halo:
            copy.wait()

        @pl.when(k > 0)
        def _():
            for copy in distant:
                copy.wait()

        for d in partners:
            if d[2] == 0:
                block = frecv[p, level_slot[d], layers_of(d[1])[0]]
                fedges[p, id_of(d), 0] = jnp.where(
                    lane[:1] < (tile - 1) * slots, block[tile - 2 : tile - 1], block[tile - 1 : tile]
                )
        parts = [fedges[p, d, 0] for d in range(devices)]
        while len(parts) > 1:
            parts = [sum(parts[i + 1 : i + 2], parts[i]) for i in range(0, len(parts), 2)]
        at = (tile - 2) * slots
        vigor = jnp.broadcast_to(parts[0][:, at : at + 1], (1, lanes))
        potential = jnp.broadcast_to(parts[0][:, lanes - slots : lanes - slots + 1], (1, lanes))
        count = jnp.broadcast_to(parts[0][:, lanes - 1 :], (1, lanes))
        warmth = 2.0 * vigor / (3.0 * count)
        lam = jnp.where(k == 0, 1.0, jnp.sqrt(1.0 + BATH_STRENGTH * (GOAL_WARMTH / warmth - 1.0)))
        which = lax.broadcasted_iota(jnp.int32, (2, lanes), 1)
        record = jnp.concatenate([potential, lam * lam * vigor], axis=0) / slot_total
        history[...] = jnp.where(which == k - 1, record, history[...])
        before = jnp.where(k > 0, half, 0.0)

        @pl.when(k < STEPS)
        def _():
            found = columns(
                lambda yl: fsend[p, yl], lambda s, yl: frecv[p, s, yl],
                lambda d, at: fedges[p, id_of(d), at],
            )
            for (xi, py, dz), f in found.items():
                f = jnp.where(tile_row < 3 * nx, f, 0.0)
                v = (vstate[xi, py, dz] + before * f) * lam
                v = v + half * f
                vstate[xi, py, dz] = v
                ostate[xi, py, dz] = ostate[xi, py, dz] + TIME_STEP * v

        @pl.when(k == STEPS)
        def _():
            for y in range(ny):
                v = (vstate[0, y + 1, 1] + half * fsend[p, y]) * lam
                result[y] = ostate[0, y + 1, 1]
                result[ny + y] = v
                result[2 * ny + y] = fsend[p, y]
            result[3 * ny, 0:2] = history[...]

        return 0

    history[...] = jnp.zeros_like(history)
    lax.fori_loop(0, STEPS + 1, step, 0)


def unpack(shape, result, o_in, occ_in, o_out, v_out, f_out, h_out):
    nx, ny, nz, slots = shape
    lanes = nz * slots
    at = lax.broadcasted_iota(jnp.int32, (nz, lanes), 0) * slots + lax.rem(
        lax.broadcasted_iota(jnp.int32, (nz, lanes), 1), slots
    )
    for i, ref in enumerate((o_out, v_out, f_out)):
        for y in range(ny):
            for x in range(nx):
                for c in range(3):
                    r = c * nx + x
                    row = jnp.broadcast_to(result[i * ny + y, r : r + 1], (nz, lanes))
                    plane = jnp.take_along_axis(row, at, axis=1, mode="promise_in_bounds")[:, :slots]
                    if i == 0:
                        plane = jnp.where(occ_in[x, y] > 0, plane, o_in[x, y, c])
                    ref[x, y, c] = plane
    h_out[...] = result[3 * ny, 0:2, :STEPS]


def shards(axes, offsets, velocities, occupied):
    gx, gy, gz = axes
    nx, ny, nz, slots = occupied.shape
    lanes = nz * slots
    tile = lanes // slots
    assert gz > 2 and tile >= 3 * nx + 2
    nxo, nyo, nzo = (len(offsets_of(s)) for s in axes)
    halo = nxo * nyo * nzo - 1
    level = nxo * nyo - 1
    devices = gx * gy * gz
    f32 = jnp.float32
    plane = jax.ShapeDtypeStruct((nx, ny, 3, nz, slots), f32)
    vmem = pl.BlockSpec(memory_space=pltpu.VMEM)
    dma = pltpu.SemaphoreType.DMA
    o_planes = jnp.transpose(offsets, (0, 1, 4, 2, 3))
    result = pl.pallas_call(
        functools.partial(kernel, axes, (nx, ny, nz, slots)),
        name="verlet",
        out_shape=jax.ShapeDtypeStruct((3 * ny + 1, tile, lanes), f32),
        in_specs=[vmem] * 3,
        out_specs=vmem,
        scratch_shapes=[
            pltpu.VMEM((nxo, ny + 2, 3, tile, lanes), f32),
            pltpu.VMEM((nxo, ny + 2, 3, tile, lanes), f32),
            pltpu.VMEM((nx + 2, ny + 2, 3, 3, slots, lanes), f32),
            pltpu.VMEM((ny, 2, tile, lanes), f32),
            pltpu.VMEM((max(level, 1), ny, 2, tile, lanes), f32),
            pltpu.VMEM((2, ny, 2, 1, lanes), f32),
            pltpu.VMEM((halo, ny, 2, 1, lanes), f32),
            pltpu.VMEM((2, ny, tile, lanes), f32),
            pltpu.VMEM((2, max(level, 1), ny, tile, lanes), f32),
            pltpu.VMEM((2, 2, ny, 1, lanes), f32),
            pltpu.VMEM((2, devices, ny, 1, lanes), f32),
            pltpu.VMEM((1, lanes), f32),
            pltpu.VMEM((2, lanes), f32),
            dma((halo,)),
            dma((halo,)),
            dma((devices - 1,)),
            dma((2, devices - 1)),
        ],
        compiler_params=pltpu.CompilerParams(collective_id=0, has_side_effects=True),
    )(
        o_planes,
        jnp.transpose(velocities, (0, 1, 4, 2, 3)),
        occupied,
    )
    o, v, f, h = pl.pallas_call(
        functools.partial(unpack, (nx, ny, nz, slots)),
        name="unpack",
        out_shape=[plane, plane, plane, jax.ShapeDtypeStruct((2, STEPS), f32)],
        in_specs=[vmem] * 3,
        out_specs=[vmem] * 4,
    )(result, o_planes, occupied)
    back = (0, 1, 3, 4, 2)
    return (jnp.transpose(o, back), jnp.transpose(v, back), jnp.transpose(f, back), h.T)


def solution(mesh):
    axes = tuple(mesh.shape[a] for a in ("gx", "gy", "gz"))
    in_specs = (
        P("gx", "gy", "gz", None, None),
        P("gx", "gy", "gz", None, None),
        P("gx", "gy", "gz", None),
    )
    out_specs = (
        P("gx", "gy", "gz", None, None),
        P("gx", "gy", "gz", None, None),
        P("gx", "gy", "gz", None, None),
        P(),
    )
    return jax.shard_map(
        functools.partial(shards, axes), mesh=mesh, in_specs=in_specs, out_specs=out_specs, check_vma=False
    )
```
